32 devices in a mesh: ctx: 16 (over z, x, core), fsdp: 2 (over y).
Axes of the slice: x: 2, y: 2, z: 4, core: 2. Of those that a mesh axis runs over, the one named last changes fastest.
Arguments:
- layer_input: bfloat16 [2048, 4096], P('ctx'), may hold values from -8 to 8
- gain: float32 [4096], replicated, may hold values from 0.5 to 1.5
- codes: int32 [4096, 384], P('fsdp'), may hold values from -2147483648 to 2147483646
- column_scale_quantized: int32 [64, 3072], P('fsdp'), may hold values from 0 to 255
- block_second_scale: float32 [64], replicated, may hold values from 0.03 to 0.12
- query_down_map: bfloat16 [4096, 16], replicated, may hold values from -0.09375 to 0.09375
- query_up_map: bfloat16 [16, 2048], P(None, 'fsdp'), may hold values from -0.29882812 to 0.29882812
- token_document: int32 [2048], P('ctx'), may hold values from 0 to 3, as said below
- output_cotangent: bfloat16 [2048, 2048], P('ctx', 'fsdp'), may hold values from -0.059814453 to 0.059814453
Outputs:
- attn: bfloat16 [2048, 2048], P('ctx', 'fsdp')
- grad_a: float32 [4096, 16], replicated
- up_map_gradient: float32 [16, 2048], P(None, 'fsdp')
The draws below stay inside these ranges and needn't reach their ends.
Inputs may be any that keep to these rules, and one draw needn't show every extreme that they name: token_document never falls along the sequence; each document has 1 to 1536 tokens and one has exactly 1536.
All inputs are finite; a program needn't handle non-finite values.
Results may differ from the reference program's by a relative error of at most 0.028.
Values may be sent and summed in bfloat16 or wider, within the bound.
A program may use at most 192 MiB of HBM per device.

```python
import math
import jax
import jax.numpy as jnp
import numpy as np
from jax import lax

MODEL_WIDTH = 4096
QUERY_HEADS = 16
KEY_VALUE_HEADS = 4
HEAD_SIZE = 128
ADAPTER_RANK = 16
DOCS = 4
SEQUENCE_TOKENS = 2048
MOST = 1536
QUERY_FEATURES = 2048
COLS = 3072
N_FSDP = 2


NF4_LEVELS = [-1.0, -0.6961928009986877, -0.5250730514526367, -0.39491748809814453, -0.28444138169288635, -0.18477343022823334, -0.09105003625154495, 0.0, 0.07958029955625534, 0.16093020141124725, 0.24611230194568634, 0.33791524171829224, 0.44070982933044434, 0.5626170039176941, 0.7229568362236023, 1.0]


def weight_parts(key):
    code_key = jax.random.fold_in(key, 101)
    scale_key = jax.random.fold_in(key, 102)
    const_key = jax.random.fold_in(key, 103)
    packed = jax.random.randint(code_key, (MODEL_WIDTH, COLS // 8), -2147483648, 2147483647, dtype=jnp.int32)
    scales = jax.random.randint(scale_key, (MODEL_WIDTH // 64, COLS), 0, 256, dtype=jnp.int32)
    lower, upper = (0.03, 0.09)
    consts = jnp.exp(jax.random.uniform(const_key, (MODEL_WIDTH // 64,), jnp.float32, math.log(lower), math.log(upper)))
    return (packed, scales, consts)


def unpack_weights(packed, scales, consts):
    row_count = packed.shape[0]
    pieces = [jnp.bitwise_and(jnp.right_shift(packed, 4 * nibble), 15) for nibble in range(8)]
    unpacked = jnp.stack(pieces, axis=-1).reshape(row_count, packed.shape[1] * 8)
    table = jnp.asarray(NF4_LEVELS, jnp.float32)
    levels = table[unpacked]
    absmax = (scales.astype(jnp.float32) + 1.0) / 256.0 * consts[:, None]
    return (levels.reshape(row_count // 64, 64, -1) * absmax[:, None, :]).reshape(row_count, -1)


def doc_layout(key):
    layout_key = jax.random.fold_in(key, 401)
    long_slot = jax.random.randint(jax.random.fold_in(layout_key, 1), (), 1, DOCS, dtype=jnp.int32)
    remaining = jnp.int32(SEQUENCE_TOKENS - MOST)
    others = []
    for number in range(DOCS - 2):
        upper_len = remaining - (DOCS - 2 - number) + 1
        length_now = jax.random.randint(jax.random.fold_in(layout_key, 10 + number), (), 1, upper_len, dtype=jnp.int32)
        others.append(length_now)
        remaining = remaining - length_now
    others.append(remaining)
    lengths = []
    for number in range(DOCS):
        before = others[min(number, DOCS - 2)]
        after = others[max(number - 1, 0)]
        lengths.append(jnp.where(number < long_slot, before, jnp.where(number == long_slot, jnp.int32(MOST), after)))
    lengths = jnp.stack(lengths).astype(jnp.int32)
    ends = jnp.cumsum(lengths).astype(jnp.int32)
    positions = jnp.arange(SEQUENCE_TOKENS, dtype=jnp.int32)
    ids = jnp.sum((positions[:, None] >= ends[None, :DOCS - 1]).astype(jnp.int32), axis=1).astype(jnp.int32)
    starts = ends - lengths
    long_start = jnp.sum(jnp.where(jnp.arange(DOCS, dtype=jnp.int32) == long_slot, starts, 0)).astype(jnp.int32)
    return (ids, long_start)


def draw_token_document(key, part):
    return doc_layout(key)[0]


def draw_codes(key, part):
    return weight_parts(key)[0]


def draw_column_scale_quantized(key, part):
    return weight_parts(key)[1]


def draw_block_second_scale(key, part):
    return weight_parts(key)[2]


def far_pairs(key, fields, weight):
    long_start = doc_layout(key)[1]
    hq_local = QUERY_HEADS // N_FSDP
    key_value_local = KEY_VALUE_HEADS // N_FSDP
    group_columns = COLS // N_FSDP
    head_grouped = QUERY_HEADS // KEY_VALUE_HEADS
    half_size = HEAD_SIZE // 2
    edge_dims = max(HEAD_SIZE // 16, 1)
    aligned = list(range(half_size - edge_dims, half_size)) + list(range(HEAD_SIZE - edge_dims, HEAD_SIZE))
    root_width = math.sqrt(MODEL_WIDTH)
    for plant in range(8):
        query_head = 3 * plant % QUERY_HEADS
        group_id = query_head // hq_local
        key_head = query_head // head_grouped
        query_cols = np.array([group_id * group_columns + (query_head - group_id * hq_local) * HEAD_SIZE + dim for dim in aligned])
        key_cols = np.array([group_id * group_columns + hq_local * HEAD_SIZE + (key_head - group_id * key_value_local) * HEAD_SIZE + dim for dim in aligned])
        columns = jnp.concatenate([weight[:, query_cols], weight[:, key_cols]], axis=1)
        direction = jnp.sum(columns, axis=1)
        direction = direction / jnp.sqrt(jnp.sum(direction * direction))
        offset = jax.random.randint(jax.random.fold_in(key, 500 + plant), (), 0, SEQUENCE_TOKENS // 4, dtype=jnp.int32)
        position = long_start + offset
        vector = root_width * direction
        fields = fields.at[position].set(vector)
        fields = fields.at[position + SEQUENCE_TOKENS // 2].set(vector)
    return fields


def draw_layer_input(key, part):
    fields = jax.random.normal(jax.random.fold_in(key, 201), (SEQUENCE_TOKENS, MODEL_WIDTH), jnp.float32)
    packed, scales, consts = weight_parts(key)
    weight = unpack_weights(packed, scales, consts)
    fields = far_pairs(key, fields, weight)
    return jnp.clip(fields, -6.0, 6.0).astype(jnp.bfloat16)


def shard_levels(stream_key, shape, shards, low, top_value):
    level = 1.0
    for dim, shards_of in shards:
        steps = jax.random.uniform(jax.random.fold_in(jax.random.fold_in(stream_key, 6), dim), (shards_of,), jnp.float32, low / len(shards), top_value / len(shards))
        level = level * jnp.repeat(jnp.exp(steps), shape[dim] // shards_of).reshape((-1,) + (1,) * (len(shape) - 1 - dim))
    return level


def bell_draw(key, dims, width, most, cuts=(), held_as=jnp.bfloat16):
    result = jax.random.normal(key, dims, jnp.float32) * width
    if len(cuts) > 0:
        result = shard_levels(key, dims, cuts, -0.22, 0.18) * result
    return jnp.clip(result, min=-most, max=most).astype(held_as)


def setup_inputs(seed: int = 0) -> dict:
    splits = jax.random.split(jax.random.key(seed), 10)
    layer_input = draw_layer_input(jax.random.fold_in(splits[9], 71), 0)
    gain = jnp.clip(1.0 + 0.1 * jax.random.normal(splits[1], (MODEL_WIDTH,), jnp.float32), 0.5, 1.5)
    codes = draw_codes(jax.random.fold_in(splits[9], 71), 0)
    column_scale_quantized = draw_column_scale_quantized(jax.random.fold_in(splits[9], 71), 0)
    block_second_scale = draw_block_second_scale(jax.random.fold_in(splits[9], 71), 0)
    query_down_map = bell_draw(splits[5], (MODEL_WIDTH, ADAPTER_RANK), MODEL_WIDTH ** -0.5, 0.09375)
    query_up_map = bell_draw(splits[6], (ADAPTER_RANK, QUERY_FEATURES), 0.05, 0.29882812, ((1, 2),))
    token_document = draw_token_document(jax.random.fold_in(splits[9], 71), 0)
    output_cotangent = bell_draw(splits[8], (SEQUENCE_TOKENS, QUERY_FEATURES), 0.01, 0.059814453, ((0, 16), (1, 2)))
    return {"layer_input": layer_input, "gain": gain, "codes": codes, "column_scale_quantized": column_scale_quantized, "block_second_scale": block_second_scale, "query_down_map": query_down_map, "query_up_map": query_up_map, "token_document": token_document, "output_cotangent": output_cotangent}


NF4_LEVELS = [-1.0, -0.6961928009986877, -0.5250730514526367, -0.39491748809814453, -0.28444138169288635, -0.18477343022823334, -0.09105003625154495, 0.0, 0.07958029955625534, 0.16093020141124725, 0.24611230194568634, 0.33791524171829224, 0.44070982933044434, 0.5626170039176941, 0.7229568362236023, 1.0]
ADAPTER_SCALE = 2.0
ROPE_BASE = 500000.0

def dequantize(packed, column_scale_quantized, block_second_scale):
    row_count = packed.shape[0]
    pieces = [jnp.bitwise_and(jnp.right_shift(packed, 4 * nibble), 15) for nibble in range(8)]
    unpacked = jnp.stack(pieces, axis=-1).reshape(row_count, packed.shape[1] * 8)
    levels = jnp.zeros(unpacked.shape, jnp.float32)
    for slot_code, level_value in enumerate(NF4_LEVELS):
        levels = levels + jnp.where(unpacked == slot_code, jnp.float32(level_value), jnp.float32(0.0))
    absmax = (column_scale_quantized.astype(jnp.float32) + 1.0) / 256.0 * block_second_scale[:, None]
    scaled = levels.reshape(row_count // 64, 64, -1) * absmax[:, None, :]
    return scaled.reshape(row_count, -1).astype(jnp.bfloat16)

def rope_angles(positions):
    freqs = jnp.exp(jnp.arange(HEAD_SIZE // 2, dtype=jnp.float32) * (-2.0 * math.log(ROPE_BASE) / HEAD_SIZE))
    angle = positions.astype(jnp.float32)[:, None] * freqs[None, :]
    cosine = jnp.concatenate([jnp.cos(angle), jnp.cos(angle)], axis=-1)
    sine = jnp.concatenate([jnp.sin(angle), jnp.sin(angle)], axis=-1)
    return (cosine, sine)

def apply_rotation(field, rotary_phases):
    cosine, sine = rotary_phases
    half = HEAD_SIZE // 2
    turned = jnp.concatenate([-field[..., half:], field[..., :half]], axis=-1)
    return field * cosine[:, None, :] + turned * sine[:, None, :]

def rotate_back(grads, rotary_phases):
    cosine, sine = rotary_phases
    half = HEAD_SIZE // 2
    scaled = grads * sine[:, None, :]
    turned = jnp.concatenate([-scaled[..., half:], scaled[..., :half]], axis=-1)
    return grads * cosine[:, None, :] - turned

def rms_norm(layer_input, gain):
    wide = layer_input.astype(jnp.float32)
    inverse = lax.rsqrt(lax.optimization_barrier(jnp.mean(wide * wide, axis=-1, keepdims=True)) + 1e-05)
    return (wide * inverse * gain[None, :]).astype(jnp.bfloat16)

def reference(layer_input, gain, codes, column_scale_quantized, block_second_scale, query_down_map, query_up_map, token_document, output_cotangent):
    input_normalized = rms_norm(layer_input, gain)
    weight = dequantize(codes, column_scale_quantized, block_second_scale)
    projection_output = jnp.dot(input_normalized.astype(jnp.float32), weight.astype(jnp.float32), preferred_element_type=jnp.float32)
    group_columns = (QUERY_HEADS + 2 * KEY_VALUE_HEADS) * HEAD_SIZE // N_FSDP
    q_local = QUERY_HEADS // N_FSDP * HEAD_SIZE
    key_value_local = KEY_VALUE_HEADS // N_FSDP * HEAD_SIZE
    query_slices, key_slices, value_slices = ([], [], [])
    for member in range(N_FSDP):
        anchor = member * group_columns
        query_slices.append(projection_output[:, anchor:anchor + q_local])
        key_slices.append(projection_output[:, anchor + q_local:anchor + q_local + key_value_local])
        value_slices.append(projection_output[:, anchor + q_local + key_value_local:anchor + group_columns])
    rank_reduced = jnp.dot(input_normalized.astype(jnp.float32), query_down_map.astype(jnp.float32), preferred_element_type=jnp.float32).astype(jnp.bfloat16)
    query_complete = jnp.concatenate(query_slices, axis=1) + ADAPTER_SCALE * jnp.dot(rank_reduced.astype(jnp.float32), query_up_map.astype(jnp.float32), preferred_element_type=jnp.float32)
    positions = jnp.arange(SEQUENCE_TOKENS, dtype=jnp.int32)
    rotary_phases = rope_angles(positions)
    query_rows = apply_rotation(query_complete.reshape(SEQUENCE_TOKENS, QUERY_HEADS, HEAD_SIZE), rotary_phases).astype(jnp.bfloat16)
    key_rows = apply_rotation(jnp.concatenate(key_slices, axis=1).reshape(SEQUENCE_TOKENS, KEY_VALUE_HEADS, HEAD_SIZE), rotary_phases).astype(jnp.bfloat16)
    value_rows = jnp.concatenate(value_slices, axis=1).reshape(SEQUENCE_TOKENS, KEY_VALUE_HEADS, HEAD_SIZE).astype(jnp.bfloat16)
    head_grouped = QUERY_HEADS // KEY_VALUE_HEADS
    query_grouped = query_rows.reshape(SEQUENCE_TOKENS, KEY_VALUE_HEADS, head_grouped, HEAD_SIZE).astype(jnp.float32)
    grouped_gradient = output_cotangent.reshape(SEQUENCE_TOKENS, KEY_VALUE_HEADS, head_grouped, HEAD_SIZE).astype(jnp.float32)
    keys_wide = key_rows.astype(jnp.float32)
    values_wide = value_rows.astype(jnp.float32)
    soft_scale = 1.0 / math.sqrt(HEAD_SIZE)
    block = math.gcd(SEQUENCE_TOKENS, 256)

    def one_block(block_id):
        start = (block_id * block).astype(jnp.int32)
        query_blk = lax.dynamic_slice_in_dim(query_grouped, start, block, 0)
        grad_blk = lax.dynamic_slice_in_dim(grouped_gradient, start, block, 0)
        ids_blk = lax.dynamic_slice_in_dim(token_document, start, block, 0)
        pos_blk = start + jnp.arange(block, dtype=jnp.int32)
        allowed = (ids_blk[:, None] == token_document[None, :]) & (positions[None, :] <= pos_blk[:, None])
        scores = jnp.einsum('bhgd,shd->hgbs', query_blk, keys_wide) * soft_scale
        masked = jnp.where(allowed, scores, -1e+30)
        top = lax.optimization_barrier(jnp.max(masked, axis=-1, keepdims=True))
        expo = jnp.where(allowed, jnp.exp(masked - top), 0.0)
        probs = expo / lax.optimization_barrier(jnp.sum(expo, axis=-1, keepdims=True))
        rounded = probs.astype(jnp.bfloat16).astype(jnp.float32)
        output = jnp.einsum('hgbs,shd->bhgd', rounded, values_wide)
        grad_dots = jnp.einsum('bhgd,shd->hgbs', grad_blk, values_wide)
        mean_dot = lax.optimization_barrier(jnp.sum(probs * grad_dots, axis=-1, keepdims=True))
        grad_scores = (probs * (grad_dots - mean_dot)).astype(jnp.bfloat16).astype(jnp.float32)
        grad_query = jnp.einsum('hgbs,shd->bhgd', grad_scores, keys_wide) * soft_scale
        return (output, grad_query)
    outputs, grad_queries = lax.map(one_block, jnp.arange(SEQUENCE_TOKENS // block, dtype=jnp.int32))
    attn = outputs.reshape(SEQUENCE_TOKENS, QUERY_HEADS * HEAD_SIZE).astype(jnp.bfloat16)
    linear_gradient = rotate_back(grad_queries.reshape(SEQUENCE_TOKENS, QUERY_HEADS, HEAD_SIZE), rotary_phases).reshape(SEQUENCE_TOKENS, QUERY_HEADS * HEAD_SIZE).astype(jnp.bfloat16)
    up_map_gradient = ADAPTER_SCALE * jnp.dot(rank_reduced.T.astype(jnp.float32), linear_gradient.astype(jnp.float32), preferred_element_type=jnp.float32)
    middle_gradient = (ADAPTER_SCALE * jnp.dot(linear_gradient.astype(jnp.float32), query_up_map.T.astype(jnp.float32), preferred_element_type=jnp.float32)).astype(jnp.bfloat16)
    grad_a = jnp.dot(input_normalized.T.astype(jnp.float32), middle_gradient.astype(jnp.float32), preferred_element_type=jnp.float32)
    return (attn, grad_a, up_map_gradient)
```

```python
import math
import functools

import jax
import jax.numpy as jnp
from jax import lax
from jax.experimental import pallas as pl
from jax.experimental.pallas import tpu as pltpu
from jax.sharding import PartitionSpec as P

QUERY_HEADS = 16
KEY_VALUE_HEADS = 4
HEAD_SIZE = 128
ADAPTER_SCALE = 2.0
ROPE_BASE = 500000.0
ID_ROWS = 16
MESH = pl.DeviceIdType.MESH
F32 = jnp.float32
BF16 = jnp.bfloat16

NF4_LEVELS = [
    -1.0,
    -0.6961928009986877,
    -0.5250730514526367,
    -0.39491748809814453,
    -0.28444138169288635,
    -0.18477343022823334,
    -0.09105003625154495,
    0.0,
    0.07958029955625534,
    0.16093020141124725,
    0.24611230194568634,
    0.33791524171829224,
    0.44070982933044434,
    0.5626170039176941,
    0.7229568362236023,
    1.0,
]


def take_lanes(values, index):
    return jnp.take_along_axis(values, index, axis=1, mode="promise_in_bounds")


def nt(a, b):
    return lax.dot_general(a, b, (((1,), (1,)), ((), ())), preferred_element_type=F32)


def tn(a, b):
    return lax.dot_general(a, b, (((0,), (0,)), ((), ())), preferred_element_type=F32)


def proj_kernel(
    x_ref, gain_ref, codes_ref, cs_ref, bss_ref, qdown_ref, qup_ref, ids_ref, cos_ref, sin_ref,
    q_ref, kv_ref, xn_ref, lr_ref,
    scl, vscl, acc, acct, own_kv, send_kv, recv_kv, send_q, recv_q, send_sem, recv_sem,
):
    member = lax.axis_index("fsdp")
    partner = 1 - member
    rows = x_ref.shape[0]
    width = x_ref.shape[1]
    depth = codes_ref.shape[0]
    blocks = cs_ref.shape[0]
    block_rows = depth // blocks
    half_lanes = 64

    barrier = pltpu.get_barrier_semaphore()
    pl.semaphore_signal(barrier, inc=1, device_id={"fsdp": partner}, device_id_type=MESH)
    pl.semaphore_wait(barrier, 1)

    lane = lax.broadcasted_iota(jnp.int32, (blocks, 128), 1)
    second = bss_ref[pl.ds(pl.multiple_of(member * blocks, 8), blocks), :]
    for tile in range(3):
        source = [
            (cs_ref[:, tile * 1024 + m * 128 : tile * 1024 + (m + 1) * 128].astype(F32) + 1.0)
            / 256.0
            * second
            for m in range(8)
        ]
        for n in range(8):
            index = 8 * (lane % 16) + n
            picked = take_lanes(source[0], index)
            for m in range(1, 8):
                picked = jnp.where(lane // 16 == m, take_lanes(source[m], index), picked)
            scl[tile * 8 + n] = picked

    for r in range(0, rows, 16):
        wide = x_ref[r : r + 16, :].astype(F32)
        inverse = lax.rsqrt(jnp.mean(wide * wide, axis=-1, keepdims=True) + 1e-05)
        xn_ref[r : r + 16, :] = (wide * inverse * gain_ref[...]).astype(BF16)
    lr_t = nt(qdown_ref[...], xn_ref[...]).astype(BF16)
    lr_ref[...] = lr_t

    level_lane = lax.broadcasted_iota(jnp.int32, (block_rows, 128), 1)
    table = jnp.zeros((block_rows, 128), F32)
    for code, level in enumerate(NF4_LEVELS):
        table = jnp.where(level_lane % 16 == code, F32(level), table)
    low_lanes = level_lane < half_lanes

    pr = lax.broadcasted_iota(jnp.int32, (128, 128), 0)
    pd = lax.broadcasted_iota(jnp.int32, (128, 128), 1)
    perm = (pd == 8 * (pr % 16) + pr // 16).astype(F32).astype(BF16)

    chunk = 512
    per_chunk = chunk // block_rows

    def phase(low_tile, high_tile):
        low_at = pl.multiple_of(low_tile * 128, 128)
        high_at = pl.multiple_of(high_tile * 128, 128)
        for n in range(8):
            vscl[n] = jnp.where(
                lane < half_lanes, scl[low_tile * 8 + n], scl[high_tile * 8 + n]
            )
        acc[...] = jnp.zeros_like(acc)

        def step(k, carry):
            lhs = xn_ref[:, pl.ds(pl.multiple_of(member * depth + k * chunk, 128), chunk)]
            words = []
            for b in range(per_chunk):
                at = pl.multiple_of(k * chunk + b * block_rows, block_rows)
                words.append(
                    jnp.where(
                        low_lanes,
                        codes_ref[pl.ds(at, block_rows), pl.ds(low_at, 128)],
                        codes_ref[pl.ds(at, block_rows), pl.ds(high_at, 128)],
                    )
                )
            for pair in range(4):
                planes = []
                for n in (2 * pair, 2 * pair + 1):
                    pieces = []
                    for b in range(per_chunk):
                        code = jnp.bitwise_and(jnp.right_shift(words[b], 4 * n), 15)
                        scale = vscl[n, pl.ds(k * per_chunk + b, 1), :]
                        pieces.append((take_lanes(table, code) * scale).astype(BF16))
                    planes.append(jnp.concatenate(pieces, axis=0))
                weight = jnp.concatenate(planes, axis=1)
                acc[:, pair * 256 : (pair + 1) * 256] += jnp.dot(
                    lhs, weight, preferred_element_type=F32
                )
            return carry

        lax.fori_loop(0, depth // chunk, step, 0)

    def turn(out):
        for n in range(8):
            out[n] = acc[:, n * 128 : (n + 1) * 128].T

    def exchange(src, dst, number):
        copy = pltpu.make_async_remote_copy(
            src_ref=src,
            dst_ref=dst,
            send_sem=send_sem.at[number],
            recv_sem=recv_sem.at[number],
            device_id={"fsdp": partner},
            device_id_type=MESH,
        )
        copy.start()
        return copy

    phase(1, 2)
    turn(acct)
    own_at = pl.multiple_of(member * 64, 64)
    other_at = pl.multiple_of(partner * 64, 64)
    send_kv[...] = acct[:, pl.ds(other_at, 64), :].astype(BF16)
    copy_kv = exchange(send_kv, recv_kv, 0)
    own_kv[...] = acct[:, pl.ds(own_at, 64), :]

    phase(2 * partner, partner)
    turn(acct)
    send_q[...] = acct[...].astype(BF16)
    copy_q = exchange(send_q, recv_q, 1)

    cosine = cos_ref[...].reshape(8, 8, rows)
    sine = sin_ref[...].reshape(8, 8, rows)

    def rotate(field):
        a, b = field[:, :8, :], field[:, 8:, :]
        return jnp.concatenate([a * cosine - b * sine, b * cosine + a * sine], axis=1)

    def natural(field):
        return tn(field.reshape(128, rows).astype(BF16), perm).astype(BF16)

    copy_kv.wait()
    for head in range(2):
        k_at, v_at = 16 * head, 32 + 16 * head
        key = own_kv[:, k_at : k_at + 16, :] + recv_kv[:, k_at : k_at + 16, :].astype(F32)
        kv_ref[:rows, head * 256 : head * 256 + 128] = natural(rotate(key))
        value = own_kv[:, v_at : v_at + 16, :] + recv_kv[:, v_at : v_at + 16, :].astype(F32)
        kv_ref[:rows, head * 256 + 128 : head * 256 + 256] = natural(value)
    ids = jnp.broadcast_to(ids_ref[...].astype(F32), (ID_ROWS, rows)).astype(BF16)
    kv_ref[rows:, :] = jnp.concatenate([ids] * 4, axis=1)

    phase(2 * member, member)
    turn(acct)
    copy_q.wait()
    for head in range(8):
        at = pl.multiple_of(16 * lax.rem(head + 4 * member, 8), 16)
        up_t = nt(perm, qup_ref[:, head * 128 : (head + 1) * 128]).astype(BF16)
        adapter = jnp.dot(up_t, lr_t, preferred_element_type=F32).reshape(8, 16, rows)
        query = acct[:, pl.ds(at, 16), :] + recv_q[:, pl.ds(at, 16), :].astype(F32)
        query = query + ADAPTER_SCALE * adapter
        q_ref[:, head * 128 : (head + 1) * 128] = natural(rotate(query))


def attn_kernel(
    first_ref, q_ref, do_ref, kv_ref, ids_ref, xn_ref, lr_ref, qup_ref, cos_ref, sin_ref,
    out_ref, up_ref, ga_ref,
    qs, dos, row_max, row_sum, row_dot, out_acc, grad_acc, lin,
):
    me = lax.axis_index("ctx")
    rows = q_ref.shape[0]
    soft_scale = 1.0 / math.sqrt(HEAD_SIZE)
    group = QUERY_HEADS // KEY_VALUE_HEADS
    many = group * rows
    my_ids = ids_ref[...]

    for head in range(8):
        at = head * rows
        qs[at : at + rows, :] = q_ref[:, head * 128 : (head + 1) * 128]
        dos[at : at + rows, :] = do_ref[:, head * 128 : (head + 1) * 128]

    def part(head, kv_part, allowed, first):
        span = pl.ds(head * many, many)
        key = kv_part[:, head * 256 : head * 256 + 128]
        value = kv_part[:, head * 256 + 128 : head * 256 + 256]
        both = kv_part[:, head * 256 : head * 256 + 256]
        scores = nt(qs[span, :], key) * soft_scale
        scores = jnp.where(jnp.concatenate([allowed] * group, axis=0), scores, -1e30)
        top = jnp.max(scores, axis=-1, keepdims=True)
        if not first:
            top = jnp.maximum(top, row_max[span, :])
        expo = jnp.exp(scores - top)
        weighted = expo * nt(dos[span, :], value)
        total = jnp.sum(expo, axis=-1, keepdims=True)
        dot_total = jnp.sum(weighted, axis=-1, keepdims=True)
        new_out = jnp.dot(expo.astype(BF16), both, preferred_element_type=F32)
        new_grad = jnp.dot(weighted.astype(BF16), key, preferred_element_type=F32)
        if first:
            row_sum[span, :] = total
            row_dot[span, :] = dot_total
            out_acc[span, :] = new_out
            grad_acc[span, :] = new_grad
        else:
            decay = jnp.exp(row_max[span, :] - top)
            row_sum[span, :] = decay * row_sum[span, :] + total
            row_dot[span, :] = decay * row_dot[span, :] + dot_total
            out_acc[span, :] = decay * out_acc[span, :] + new_out
            grad_acc[span, :] = decay * grad_acc[span, :] + new_grad
        row_max[span, :] = top

    diag = kv_ref[me]
    key_ids = diag[rows : rows + 1, :128].astype(F32)
    qi = lax.broadcasted_iota(jnp.int32, (rows, rows), 0)
    ki = lax.broadcasted_iota(jnp.int32, (rows, rows), 1)
    allowed = (my_ids == key_ids) & (ki <= qi)
    for head in range(2):
        part(head, diag[:rows], allowed, True)

    lane = lax.broadcasted_iota(jnp.int32, (1, 2 * rows), 1)

    def step(t, carry):
        upper = me - 2 * t
        start = jnp.maximum(upper - 2, 0)
        pair = [kv_ref[start], kv_ref[start + 1]]
        both = jnp.concatenate([p[:rows] for p in pair], axis=0)
        key_ids = jnp.concatenate([p[rows : rows + 1, :128] for p in pair], axis=1).astype(F32)
        key_ids = jnp.where(lane < (upper - start) * rows, key_ids, -1.0)
        allowed = my_ids == key_ids
        for head in range(2):
            part(head, both, allowed, False)
        return carry

    lax.fori_loop(0, (me - first_ref[0] + 1) // 2, step, 0)

    cosine, sine = cos_ref[...], sin_ref[...]
    for head in range(8):
        at = head * rows
        span = slice(at, at + rows)
        inverse = 1.0 / row_sum[span, :]
        out_ref[:, head * 128 : (head + 1) * 128] = (out_acc[span, 128:] * inverse).astype(BF16)
        mean_dot = row_dot[span, :] * inverse
        grad = soft_scale * inverse * (grad_acc[span, :] - mean_dot * out_acc[span, :128])
        turned = pltpu.roll(grad * sine, 64, 1)
        lin[:, head * 128 : (head + 1) * 128] = (grad * cosine + turned).astype(BF16)
    up_ref[...] = ADAPTER_SCALE * jnp.dot(lr_ref[...], lin[...], preferred_element_type=F32)
    middle = (ADAPTER_SCALE * nt(qup_ref[...], lin[...])).astype(BF16)
    ga_ref[...] = jnp.dot(middle, xn_ref[...], preferred_element_type=F32)


def reduce_kernel(
    counts, ga_ref, up_ref, ga_out, up_out,
    ga_part, ga_in, ga_sum, ga_all, up_part, up_in, up_sum, up_all, sems,
):
    ctx_count, fsdp_count = counts
    total = ctx_count * fsdp_count
    ctx, fsdp = lax.axis_index("ctx"), lax.axis_index("fsdp")
    me = ctx * fsdp_count + fsdp
    ga_owners, up_owners = ga_part.shape[0], up_part.shape[0]
    ga_stride, up_stride = total // ga_owners, ctx_count // up_owners
    tiles = up_owners // 2

    barrier = pltpu.get_barrier_semaphore()

    def greet(step, carry):
        other = lax.rem(me + step, total)
        pl.semaphore_signal(
            barrier, inc=1, device_id=(other // fsdp_count, lax.rem(other, fsdp_count)),
            device_id_type=MESH,
        )
        return carry

    lax.fori_loop(1, total, greet, 0)

    for j in range(ga_owners):
        ga_part[j] = ga_ref[:, j * 128 : (j + 1) * 128].astype(BF16)
    for j in range(up_owners):
        row, col = 8 * (j // tiles), 128 * (j % tiles)
        up_part[j] = up_ref[row : row + 8, col : col + 128]
    pl.semaphore_wait(barrier, total - 1)

    def send(src, dst, number, ctx_to, fsdp_to):
        pltpu.make_async_remote_copy(
            src_ref=src, dst_ref=dst, send_sem=sems.at[2 * number],
            recv_sem=sems.at[2 * number + 1], device_id=(ctx_to, fsdp_to),
            device_id_type=MESH,
        ).start()

    def keep(src, dst, number):
        pltpu.make_async_copy(src, dst, sems.at[2 * number + 1]).start()

    def await_all(buffer, number, slot):
        pltpu.make_async_copy(buffer, buffer, sems.at[2 * number + slot]).wait()

    up_mine, ga_mine = ctx // up_stride, me // ga_stride
    up_owner, ga_owner = lax.rem(ctx, up_stride) == 0, lax.rem(me, ga_stride) == 0

    def scatter_up(step, carry):
        j = lax.rem(up_mine + step, up_owners)
        to = j * up_stride

        @pl.when(to != ctx)
        def _():
            send(up_part.at[j], up_in.at[ctx], 0, to, fsdp)

        return carry

    def scatter_ga(step, carry):
        j = lax.rem(ga_mine + step, ga_owners)
        to = j * ga_stride

        @pl.when(to != me)
        def _():
            send(
                ga_part.at[j], ga_in.at[me], 1, to // fsdp_count, lax.rem(to, fsdp_count)
            )

        return carry

    lax.fori_loop(0, up_owners, scatter_up, 0)
    lax.fori_loop(0, ga_owners, scatter_ga, 0)

    @pl.when(up_owner)
    def _():
        keep(up_part.at[up_mine], up_in.at[ctx], 0)
        await_all(up_in, 0, 1)
        up_sum[...] = jnp.sum(up_in[...], axis=0)

        def spread(step, carry):
            send(up_sum, up_all.at[up_mine], 2, lax.rem(ctx + step, ctx_count), fsdp)
            return carry

        lax.fori_loop(1, ctx_count, spread, 0)
        keep(up_sum, up_all.at[up_mine], 2)

    @pl.when(ga_owner)
    def _():
        keep(ga_part.at[ga_mine], ga_in.at[me], 1)
        await_all(ga_in, 1, 1)
        ga_sum[...] = jnp.sum(ga_in[...].astype(F32), axis=0).astype(BF16)

        def spread(step, carry):
            to = lax.rem(me + step, total)
            send(ga_sum, ga_all.at[ga_mine], 3, to // fsdp_count, lax.rem(to, fsdp_count))
            return carry

        lax.fori_loop(1, total, spread, 0)
        keep(ga_sum, ga_all.at[ga_mine], 3)

    await_all(up_all, 2, 1)
    for j in range(up_owners):
        row, col = 8 * (j // tiles), 128 * (j % tiles)
        up_out[row : row + 8, col : col + 128] = up_all[j]
    await_all(ga_all, 3, 1)
    for j in range(ga_owners):
        ga_out[:, j * 128 : (j + 1) * 128] = ga_all[j].astype(F32)

    def drain(buffer, number, sent):
        @pl.when(sent > 0)
        def _():
            def one(step, carry):
                pltpu.make_async_copy(buffer, buffer, sems.at[2 * number]).wait()
                return carry

            lax.fori_loop(0, sent, one, 0)

    drain(up_part.at[0], 0, up_owners - up_owner.astype(jnp.int32))
    drain(ga_part.at[0], 1, ga_owners - ga_owner.astype(jnp.int32))
    drain(up_sum, 2, jnp.where(up_owner, ctx_count - 1, 0))
    drain(ga_sum, 3, jnp.where(ga_owner, total - 1, 0))


def rope_tables(place, rows):
    positions = (place * rows + jnp.arange(rows, dtype=jnp.int32)).astype(F32)
    half = HEAD_SIZE // 2
    freqs = jnp.exp(jnp.arange(half, dtype=F32) * (-2.0 * math.log(ROPE_BASE) / HEAD_SIZE))
    angle = positions[:, None] * freqs[None, :]
    cosine, sine = jnp.cos(angle), jnp.sin(angle)
    def planes(table):
        return jnp.transpose(table.T.reshape(8, 8, rows), (1, 0, 2)).reshape(half, rows)

    wide_cos = jnp.concatenate([cosine, cosine], axis=-1)
    wide_sin = jnp.concatenate([-sine, sine], axis=-1)
    return planes(cosine), planes(sine), wide_cos, wide_sin


def on_device(
    counts, layer_input, gain, codes, column_scale_quantized, block_second_scale,
    query_down_map, query_up_map, token_document, output_cotangent,
):
    rows, width = layer_input.shape
    place = lax.axis_index("ctx")
    cos_t, sin_t, cos_w, sin_w = rope_tables(place, rows)
    vm = pl.BlockSpec(memory_space=pltpu.VMEM)
    sm = pl.BlockSpec(memory_space=pltpu.SMEM)
    blocks = column_scale_quantized.shape[0]
    rank = query_up_map.shape[0]
    kv_width = 4 * HEAD_SIZE
    q, kv, xn, lr = pl.pallas_call(
        proj_kernel,
        out_shape=(
            jax.ShapeDtypeStruct((rows, query_up_map.shape[1]), BF16),
            jax.ShapeDtypeStruct((rows + ID_ROWS, kv_width), BF16),
            jax.ShapeDtypeStruct((rows, width), BF16),
            jax.ShapeDtypeStruct((rank, rows), BF16),
        ),
        in_specs=[vm] * 10,
        out_specs=(vm,) * 4,
        scratch_shapes=[
            pltpu.VMEM((24, blocks, 128), F32),
            pltpu.VMEM((8, blocks, 128), F32),
            pltpu.VMEM((rows, 1024), F32),
            pltpu.VMEM((8, 128, rows), F32),
            pltpu.VMEM((8, 64, rows), F32),
            pltpu.VMEM((8, 64, rows), BF16),
            pltpu.VMEM((8, 64, rows), BF16),
            pltpu.VMEM((8, 128, rows), BF16),
            pltpu.VMEM((8, 128, rows), BF16),
            pltpu.SemaphoreType.DMA((2,)),
            pltpu.SemaphoreType.DMA((2,)),
        ],
        compiler_params=pltpu.CompilerParams(
            collective_id=0, has_side_effects=True, vmem_limit_bytes=56 * 1024 * 1024
        ),
        name="project",
    )(
        layer_input, gain[None, :], codes, column_scale_quantized, block_second_scale[:, None],
        query_down_map.T, query_up_map, token_document[None, :], cos_t, sin_t,
    )
    all_kv = lax.all_gather(kv, "ctx", axis=0, tiled=False)
    all_ids = all_kv[:, rows, :rows].astype(F32)
    needed = (all_ids[:, -1] >= token_document[0].astype(F32)) & (
        jnp.arange(all_ids.shape[0]) <= place
    )
    first = jnp.argmax(needed).astype(jnp.int32)[None]
    heads_rows = 8 * rows
    attn, up, ga = pl.pallas_call(
        attn_kernel,
        out_shape=(
            jax.ShapeDtypeStruct(output_cotangent.shape, BF16),
            jax.ShapeDtypeStruct(query_up_map.shape, F32),
            jax.ShapeDtypeStruct((rank, width), F32),
        ),
        in_specs=[sm] + [vm] * 9,
        out_specs=(vm,) * 3,
        scratch_shapes=[
            pltpu.VMEM((heads_rows, 128), BF16),
            pltpu.VMEM((heads_rows, 128), BF16),
            pltpu.VMEM((heads_rows, 1), F32),
            pltpu.VMEM((heads_rows, 1), F32),
            pltpu.VMEM((heads_rows, 1), F32),
            pltpu.VMEM((heads_rows, 256), F32),
            pltpu.VMEM((heads_rows, 128), F32),
            pltpu.VMEM((rows, 1024), BF16),
        ],
        compiler_params=pltpu.CompilerParams(vmem_limit_bytes=56 * 1024 * 1024),
        name="attend",
    )(
        first, q, output_cotangent, all_kv, token_document.astype(F32)[:, None], xn, lr,
        query_up_map, cos_w, sin_w,
    )
    total = counts[0] * counts[1]
    ga_owners = math.gcd(total, width // 128)
    up_owners = math.gcd(counts[0], 2 * (up.shape[1] // 128))
    ga, up = pl.pallas_call(
        functools.partial(reduce_kernel, counts),
        out_shape=(
            jax.ShapeDtypeStruct((rank, width), F32),
            jax.ShapeDtypeStruct(query_up_map.shape, F32),
        ),
        in_specs=[vm] * 2,
        out_specs=(vm,) * 2,
        scratch_shapes=[
            pltpu.VMEM((ga_owners, rank, 128), BF16),
            pltpu.VMEM((total, rank, 128), BF16),
            pltpu.VMEM((rank, 128), BF16),
            pltpu.VMEM((ga_owners, rank, 128), BF16),
            pltpu.VMEM((up_owners, 8, 128), F32),
            pltpu.VMEM((counts[0], 8, 128), F32),
            pltpu.VMEM((8, 128), F32),
            pltpu.VMEM((up_owners, 8, 128), F32),
            pltpu.SemaphoreType.DMA((8,)),
        ],
        compiler_params=pltpu.CompilerParams(
            collective_id=1, has_side_effects=True, vmem_limit_bytes=56 * 1024 * 1024
        ),
        name="reduce",
    )(ga, up)
    return attn, ga.T, up


def solution(mesh):
    return jax.shard_map(
        functools.partial(on_device, (mesh.shape["ctx"], mesh.shape["fsdp"])),
        mesh=mesh,
        in_specs=(
            P("ctx", None),
            P(),
            P("fsdp", None),
            P("fsdp", None),
            P(),
            P(),
            P(None, "fsdp"),
            P("ctx"),
            P("ctx", "fsdp"),
        ),
        out_specs=(P("ctx", "fsdp"), P(), P(None, "fsdp")),
        check_vma=False,
    )
```

```python
import math
import functools

import jax
import jax.numpy as jnp
from jax import lax
from jax.experimental import pallas as pl
from jax.experimental.pallas import tpu as pltpu
from jax.sharding import PartitionSpec as P

HEAD_SIZE = 128
ADAPTER_SCALE = 2.0
ROPE_BASE = 500000.0
MESH = pl.DeviceIdType.MESH
F32 = jnp.float32
BF16 = jnp.bfloat16
I16 = jnp.int16

NF4_LEVELS = [
    -1.0,
    -0.6961928009986877,
    -0.5250730514526367,
    -0.39491748809814453,
    -0.28444138169288635,
    -0.18477343022823334,
    -0.09105003625154495,
    0.0,
    0.07958029955625534,
    0.16093020141124725,
    0.24611230194568634,
    0.33791524171829224,
    0.44070982933044434,
    0.5626170039176941,
    0.7229568362236023,
    1.0,
]


def take_lanes(values, index):
    return jnp.take_along_axis(values, index, axis=1, mode="promise_in_bounds")


def dot(a, b):
    return jnp.dot(a, b, preferred_element_type=F32)


def nt(a, b):
    return lax.dot_general(a, b, (((1,), (1,)), ((), ())), preferred_element_type=F32)


def tn(a, b):
    return lax.dot_general(a, b, (((0,), (0,)), ((), ())), preferred_element_type=F32)


def eye(size):
    row = lax.broadcasted_iota(jnp.int32, (size, size), 0)
    col = lax.broadcasted_iota(jnp.int32, (size, size), 1)
    return (row == col).astype(F32).astype(BF16)


def step_kernel(
    counts,
    x_ref, gain_ref, codes_ref, cs_ref, bss_ref, qdown_ref, qup_ref, ids_ref, cos_ref, sin_ref,
    do_ref,
    out_ref, ga_out, up_out,
    scl, vscl, acc, acct, xn, own_kv, send_kv, recv_kv, own_q, send_q, recv_q,
    do_all, ids_all, kv_all, queries, cotans, vk, row_max, out_acc, grad_acc, lin,
    out_stage, out_in,
    ga_part, ga_in, ga_sum, ga_all, up_part, up_in, up_sum, up_all,
    pair_send, pair_recv, block_send, block_recv, sems,
):
    ctx_count, fsdp_count = counts
    total = ctx_count * fsdp_count
    ctx, member = lax.axis_index("ctx"), lax.axis_index("fsdp")
    me = ctx * fsdp_count + member
    partner = 1 - member
    chip, core = ctx // 2, lax.rem(ctx, 2)
    outer, inner = chip // 2, lax.rem(chip, 2)
    sibling = ctx + 1 - 2 * core
    chips = ctx_count // 2
    rows, width = x_ref.shape
    tokens = 2 * rows
    depth = codes_ref.shape[0]
    half_depth = depth // 2
    blocks = cs_ref.shape[0]
    block_rows = depth // blocks
    half_blocks = blocks // 2

    barrier = pltpu.get_barrier_semaphore()

    def greet(step, carry):
        other = lax.rem(me + step, total)
        pl.semaphore_signal(
            barrier, inc=1, device_id=(other // fsdp_count, lax.rem(other, fsdp_count)),
            device_id_type=MESH,
        )
        return carry

    lax.fori_loop(1, total, greet, 0)

    mine_at = pl.multiple_of(core * rows, rows)
    other_at = pl.multiple_of((1 - core) * rows, rows)
    for r in range(0, rows, 16):
        wide = x_ref[r : r + 16, :].astype(F32)
        inverse = lax.rsqrt(jnp.mean(wide * wide, axis=-1, keepdims=True) + 1e-05)
        xn[pl.ds(pl.multiple_of(mine_at + r, 16), 16), :] = (
            wide * inverse * gain_ref[...]
        ).astype(BF16)
    ids_all[:, pl.ds(mine_at, rows)] = jnp.broadcast_to(
        ids_ref[...].astype(F32), (16, rows)
    ).astype(BF16)
    half_columns = do_ref.shape[1] // 2
    mine_columns = pl.multiple_of(core * half_columns, 128)
    other_columns = pl.multiple_of((1 - core) * half_columns, 128)
    do_all[pl.ds(mine_at, rows), :] = do_ref[:, pl.ds(mine_columns, half_columns)]

    pl.semaphore_wait(barrier, total - 1)

    def pair_copy(src, dst, number, device):
        copy = pltpu.make_async_remote_copy(
            src_ref=src, dst_ref=dst, send_sem=pair_send.at[number],
            recv_sem=pair_recv.at[number], device_id=device, device_id_type=MESH,
        )
        copy.start()
        return copy

    across = (sibling, member)
    beside = (ctx, partner)
    span = pl.ds(mine_at, rows)
    copy_x = pair_copy(xn.at[span], xn.at[span], 0, across)
    copy_ids = pair_copy(ids_all.at[:, span], ids_all.at[:, span], 1, across)
    copy_do = pair_copy(
        do_ref.at[:, pl.ds(other_columns, half_columns)], do_all.at[span], 2, across
    )

    lane = lax.broadcasted_iota(jnp.int32, (blocks, 128), 1)
    second = bss_ref[pl.ds(pl.multiple_of(member * blocks, 8), blocks), :]
    for tile in range(3):
        source = [
            (cs_ref[:, tile * 1024 + m * 128 : tile * 1024 + (m + 1) * 128].astype(F32) + 1.0)
            / 256.0
            * second
            for m in range(8)
        ]
        for n in range(8):
            index = 8 * (lane % 16) + n
            picked = take_lanes(source[0], index)
            for m in range(1, 8):
                picked = jnp.where(lane // 16 == m, take_lanes(source[m], index), picked)
            scl[tile * 8 + n] = picked

    pr = lax.broadcasted_iota(jnp.int32, (128, 128), 0)
    pd = lax.broadcasted_iota(jnp.int32, (128, 128), 1)
    perm = (pd == 8 * (pr % 16) + pr // 16).astype(F32).astype(BF16)
    eye_wide = eye(256)

    chunk = 512
    per_chunk = chunk // block_rows
    short_lane = lax.broadcasted_iota(jnp.int32, (block_rows, 128), 1)
    half_lane = lax.broadcasted_iota(jnp.int32, (half_blocks, 128), 1)
    long_lane = lax.broadcasted_iota(jnp.int32, (tokens, 128), 1)
    levels = [jnp.full((block_rows, 128), level, BF16) for level in NF4_LEVELS]

    def phase(paired, tile, half):
        if paired:
            shift = 16 + 96 * core

            def chosen(lanes):
                return lax.rem(lanes // 16, 2) == core

            def words_at(at):
                return jnp.where(
                    short_lane < 64,
                    codes_ref[pl.ds(at, block_rows), 128:256],
                    codes_ref[pl.ds(at, block_rows), 256:384],
                )
        else:
            shift = 64
            tile_at = pl.multiple_of(tile * 128, 128)

            def chosen(lanes):
                return lanes // 64 == half

            def words_at(at):
                return codes_ref[pl.ds(at, block_rows), pl.ds(tile_at, 128)]

        for n in range(8):
            if paired:
                scale = jnp.where(lane < 64, scl[8 + n], scl[16 + n])
            else:
                scale = scl[tile * 8 + n]
            vscl[n] = jnp.where(
                chosen(half_lane), scale[:half_blocks], pltpu.roll(scale[half_blocks:], shift, 1)
            )
        acc[...] = jnp.zeros_like(acc)
        first = chosen(short_lane)

        def step(k, carry):
            at = pl.multiple_of(member * depth + k * chunk, 128)
            lower = xn[:, pl.ds(at, chunk)]
            upper = xn[:, pl.ds(pl.multiple_of(at + half_depth, 128), chunk)]
            low_words, high_words = [], []
            for b in range(per_chunk):
                row = pl.multiple_of(k * chunk + b * block_rows, block_rows)
                words = jnp.where(
                    first,
                    words_at(row),
                    pltpu.roll(words_at(pl.multiple_of(row + half_depth, block_rows)), shift, 1),
                )
                low_words.append(words.astype(I16))
                high_words.append(jnp.right_shift(words, 16).astype(I16))
            for pair in range(4):
                planes = []
                for n in (2 * pair, 2 * pair + 1):
                    pieces = []
                    for b in range(per_chunk):
                        words = low_words[b] if n < 4 else high_words[b]
                        values = levels
                        for bit in range(4):
                            place = 4 * (n % 4) + bit
                            mark = 1 << place if place < 15 else -(1 << 15)
                            mask = (words & jnp.int16(mark)) != 0
                            values = [
                                jnp.where(mask, values[v + 1], values[v])
                                for v in range(0, len(values), 2)
                            ]
                        scale = vscl[n, pl.ds(k * per_chunk + b, 1), :]
                        pieces.append(values[0] * scale.astype(BF16))
                    planes.append(jnp.concatenate(pieces, axis=0))
                weight = jnp.concatenate(planes, axis=1)
                columns = slice(pair * 256, (pair + 1) * 256)
                acc[0, :, columns] += dot(lower, weight)
                acc[1, :, columns] += dot(upper, weight)
            return carry

        lax.fori_loop(0, half_depth // chunk, step, 0)
        keep = chosen(long_lane)
        for n in range(8):
            columns = slice(n * 128, (n + 1) * 128)
            acct[n] = jnp.where(keep, acc[0, :, columns], acc[1, :, columns]).T

    copy_x.wait()
    copy_ids.wait()
    copy_do.wait()

    def kv_field(group, part):
        at = pl.multiple_of(64 * group, 64) + 32 * part
        return acct[:, pl.ds(pl.multiple_of(at, 32), 16), :] + acct[
            :, pl.ds(pl.multiple_of(at + 16, 16), 16), :
        ]

    phase(True, 0, 0)
    for part in range(2):
        send_kv[:, 16 * part : 16 * part + 16, :] = kv_field(partner, part).astype(BF16)
    copy_kv = pair_copy(send_kv, recv_kv, 3, beside)
    for part in range(2):
        own_kv[:, 16 * part : 16 * part + 16, :] = kv_field(member, part)

    place = 3 * partner + core
    phase(False, place // 2, lax.rem(place, 2))
    send_q[...] = (acct[:, :64, :] + acct[:, 64:, :]).astype(BF16)
    copy_q = pair_copy(send_q, recv_q, 4, beside)

    place = 3 * member + core
    phase(False, place // 2, lax.rem(place, 2))
    own_q[...] = acct[:, :64, :] + acct[:, 64:, :]

    cosine = cos_ref[...].reshape(8, 8, tokens)
    sine = sin_ref[...].reshape(8, 8, tokens)

    def rotate(field):
        a, b = field[:, :8, :], field[:, 8:, :]
        return jnp.concatenate([a * cosine - b * sine, b * cosine + a * sine], axis=1)

    copy_kv.wait()
    key = own_kv[:, :16, :] + recv_kv[:, :16, :].astype(F32)
    value = own_kv[:, 16:, :] + recv_kv[:, 16:, :].astype(F32)
    fields = jnp.concatenate(
        [value.reshape(128, tokens).astype(BF16), rotate(key).reshape(128, tokens).astype(BF16)],
        axis=0,
    )
    kv_all[chip, :tokens, :] = tn(fields, eye_wide).astype(BF16)
    kv_all[chip, tokens:, :] = ids_all[...]

    def send_block(block, to_chip):
        pltpu.make_async_remote_copy(
            src_ref=kv_all.at[block], dst_ref=kv_all.at[block],
            send_sem=block_send.at[0], recv_sem=block_recv.at[block],
            device_id=(2 * to_chip + core, member), device_id_type=MESH,
        ).start()

    def await_block(block):
        pltpu.make_async_copy(kv_all.at[block], kv_all.at[block], block_recv.at[block]).wait()

    @pl.when(inner == 0)
    def _():
        send_block(chip, chip + 1)

    def along(step, carry):
        send_block(chip, chip + 2 * step)
        return carry

    lax.fori_loop(1, chips // 2 - outer, along, 0)

    lr_t = nt(qdown_ref[...], xn[...]).astype(BF16)
    my_ids = ids_all[...]
    heads = own_q.shape[1] // 16
    local = pl.multiple_of(core * heads * 128, 128)
    marks = lax.broadcasted_iota(jnp.int32, (128, tokens), 0).astype(F32)
    tags = (marks == jnp.broadcast_to(my_ids[:1].astype(F32), (128, tokens))).astype(F32)
    tags = tags.astype(BF16)
    for head in range(heads):
        columns = slice(head * tokens, (head + 1) * tokens)
        queries[128:, columns] = tags
        cotans[:, columns] = nt(perm, do_all[:, head * 128 : (head + 1) * 128]).astype(BF16)

    copy_q.wait()
    for head in range(heads):
        columns = slice(head * tokens, (head + 1) * tokens)
        up_cols = qup_ref[:, pl.ds(pl.multiple_of(local + head * 128, 128), 128)]
        adapter = dot(nt(perm, up_cols).astype(BF16), lr_t).reshape(8, 16, tokens)
        query = own_q[:, 16 * head : 16 * head + 16, :]
        query = query + recv_q[:, 16 * head : 16 * head + 16, :].astype(F32)
        query = query + ADAPTER_SCALE * adapter
        queries[:128, columns] = rotate(query).reshape(128, tokens).astype(BF16)

    soft_scale = 1.0 / math.sqrt(HEAD_SIZE)
    log_scale = soft_scale / math.log(2.0)
    tag_row = lax.broadcasted_iota(jnp.int32, (16, tokens), 0).astype(F32)
    spread_row = lax.broadcasted_iota(jnp.int32, (16, 128), 0)
    spread_lane = lax.broadcasted_iota(jnp.int32, (16, 128), 1)
    spread_tags = (spread_row == spread_lane).astype(F32).astype(BF16)
    vk[256:, :] = jnp.ones((16, tokens), BF16)

    def attend(block, diagonal):
        both = kv_all[block, :tokens, :]
        block_ids = kv_all[block, tokens:, :].astype(F32)
        barred = jnp.where(block_ids == tag_row, 0.0, -1e30).astype(BF16)
        barred = tn(barred, spread_tags).astype(BF16)
        lhs = jnp.concatenate([both[:, 128:], barred], axis=1)
        vk[:256, :] = nt(eye_wide, both).astype(BF16)
        for head in range(heads):
            columns = slice(head * tokens, (head + 1) * tokens)
            row = slice(8 * head, 8 * head + 1)
            scores = dot(lhs, queries[:, columns]) * log_scale
            if diagonal:
                ki = lax.broadcasted_iota(jnp.int32, (tokens, tokens), 0)
                qi = lax.broadcasted_iota(jnp.int32, (tokens, tokens), 1)
                scores = jnp.where(ki <= qi, scores, -1e30)
            top = jnp.max(scores, axis=0, keepdims=True)
            if not diagonal:
                before = row_max[row, :]
                top = jnp.maximum(top, before)
            expo = jnp.exp2(scores - top)
            weighted = expo * dot(both[:, :128], cotans[:, columns])
            new_out = dot(vk[...], expo.astype(BF16))
            new_grad = dot(vk[128:, :], weighted.astype(BF16))
            row_max[row, :] = top
            if diagonal:
                out_acc[head] = new_out
                grad_acc[head] = new_grad
            else:
                decay = jnp.exp2(before - top)
                out_acc[head] = decay * out_acc[head] + new_out
                grad_acc[head] = decay * grad_acc[head] + new_grad

    attend(chip, True)

    def visit(step, carry):
        place = step - inner
        odd = lax.rem(place + 2, 2) == 1
        ahead = (place + 1) // 2

        @pl.when(((step == 0) | odd) & (ahead < outer))
        def _():
            block = 2 * (outer - 1 - ahead) + inner
            await_block(block)
            send_block(block, 2 * outer + 1 - inner)

        crossed = 2 * (outer - 1 - (place - 1) // 2) + 1 - inner
        crossed = jnp.where(place < 0, chip - 1, crossed)
        column = 2 * (outer - 1 - place // 2) + inner
        block = jnp.where(odd, crossed, column)

        @pl.when(odd)
        def _():
            await_block(block)

        attend(block, False)
        return carry

    lax.fori_loop(0, chip, visit, 0)

    middle = jnp.zeros((16, tokens), F32)
    back = 16 * (pd % 8) + pd // 8
    for head in range(heads):
        inverse = 1.0 / out_acc[head, 256:257, :]
        out = (out_acc[head, :128, :] * inverse).astype(BF16)
        out_stage[:, head * 128 : (head + 1) * 128] = tn(out, perm).astype(BF16)
    mine_out = pl.ds(mine_at, rows)
    copy_out = pair_copy(out_stage.at[pl.ds(other_at, rows)], out_in, 5, across)
    out_ref[:, pl.ds(mine_columns, half_columns)] = out_stage[mine_out, :]
    up_owners = up_part.shape[0]
    half_up = up_owners // 2
    for head in range(heads):
        inverse = 1.0 / out_acc[head, 256:257, :]
        mean_dot = grad_acc[head, 128:129, :] * inverse
        grad = grad_acc[head, :128, :] - mean_dot * out_acc[head, 128:256, :]
        grad = (soft_scale * inverse * grad).reshape(8, 16, tokens)
        a, b = grad[:, :8, :], grad[:, 8:, :]
        turned = jnp.concatenate([a * cosine + b * sine, b * cosine - a * sine], axis=1)
        lin_t = turned.reshape(128, tokens).astype(BF16)
        up_cols = qup_ref[:, pl.ds(pl.multiple_of(local + head * 128, 128), 128)]
        middle = middle + dot(nt(up_cols, perm).astype(BF16), lin_t)
        up = take_lanes(ADAPTER_SCALE * nt(lr_t, lin_t), back[:16])
        up_part[2 * head] = up[:8]
        up_part[2 * head + 1] = up[8:]
    middle = (ADAPTER_SCALE * middle).astype(BF16)
    ga_owners = ga_part.shape[0]
    for j in range(ga_owners):
        ga_part[j] = dot(middle, xn[:, j * 128 : (j + 1) * 128]).astype(BF16)

    up_pieces = up_part.shape[0]
    up_stride, ga_stride = chips // up_pieces, total // ga_owners
    up_mine, ga_mine = chip // up_stride, me // ga_stride
    up_owner, ga_owner = lax.rem(chip, up_stride) == 0, lax.rem(me, ga_stride) == 0
    up_slot = core * up_pieces + up_mine

    def send(src, dst, number, ctx_to, fsdp_to):
        pltpu.make_async_remote_copy(
            src_ref=src, dst_ref=dst, send_sem=sems.at[2 * number],
            recv_sem=sems.at[2 * number + 1], device_id=(ctx_to, fsdp_to),
            device_id_type=MESH,
        ).start()

    def hold(src, dst, number):
        pltpu.make_async_copy(src, dst, sems.at[2 * number + 1]).start()

    def await_all(buffer, number):
        pltpu.make_async_copy(buffer, buffer, sems.at[2 * number + 1]).wait()

    def scatter_up(step, carry):
        j = lax.rem(up_mine + step, up_pieces)
        to = j * up_stride

        @pl.when(to != chip)
        def _():
            send(up_part.at[j], up_in.at[chip], 0, 2 * to + core, member)

        return carry

    def scatter_ga(step, carry):
        j = lax.rem(ga_mine + step, ga_owners)
        to = j * ga_stride

        @pl.when(to != me)
        def _():
            send(ga_part.at[j], ga_in.at[me], 1, to // fsdp_count, lax.rem(to, fsdp_count))

        return carry

    lax.fori_loop(0, ga_owners, scatter_ga, 0)
    lax.fori_loop(0, up_pieces, scatter_up, 0)

    copy_out.wait()
    out_ref[:, pl.ds(other_columns, half_columns)] = out_in[...]

    @pl.when(ga_owner)
    def _():
        hold(ga_part.at[ga_mine], ga_in.at[me], 1)
        await_all(ga_in, 1)
        ga_sum[...] = jnp.sum(ga_in[...].astype(F32), axis=0).astype(BF16)

        def spread(step, carry):
            to = lax.rem(me + step, total)
            send(ga_sum, ga_all.at[ga_mine], 3, to // fsdp_count, lax.rem(to, fsdp_count))
            return carry

        lax.fori_loop(1, total, spread, 0)
        hold(ga_sum, ga_all.at[ga_mine], 3)

    @pl.when(up_owner)
    def _():
        hold(up_part.at[up_mine], up_in.at[chip], 0)
        await_all(up_in, 0)
        up_sum[...] = jnp.sum(up_in[...], axis=0)

        def spread(step, carry):
            send(up_sum, up_all.at[up_slot], 2, lax.rem(ctx + step, ctx_count), member)
            return carry

        lax.fori_loop(1, ctx_count, spread, 0)
        hold(up_sum, up_all.at[up_slot], 2)

    await_all(ga_all, 3)
    for j in range(ga_owners):
        ga_out[:, j * 128 : (j + 1) * 128] = ga_all[j].astype(F32)
    await_all(up_all, 2)
    for j in range(2 * up_pieces):
        for part in range(up_all.shape[1] // 8):
            piece = j * (up_all.shape[1] // 8) + part
            row, col = 8 * (piece % 2), 128 * (piece // 2)
            up_out[row : row + 8, col : col + 128] = up_all[j, 8 * part : 8 * part + 8, :]

    def drain(buffer, semaphore, sent):
        def one(step, carry):
            pltpu.make_async_copy(buffer, buffer, semaphore).wait()
            return carry

        lax.fori_loop(0, sent, one, 0)

    passed = chips // 2 - 1 - outer + outer + 1 - inner
    drain(kv_all.at[chip], block_send.at[0], passed)
    drain(up_part.at[0], sems.at[0], up_pieces - up_owner.astype(jnp.int32))
    drain(ga_part.at[0], sems.at[2], ga_owners - ga_owner.astype(jnp.int32))
    drain(up_sum, sems.at[4], jnp.where(up_owner, ctx_count - 1, 0))
    drain(ga_sum, sems.at[6], jnp.where(ga_owner, total - 1, 0))


def rope_tables(place, tokens):
    positions = (place * tokens + jnp.arange(tokens, dtype=jnp.int32)).astype(F32)
    half = HEAD_SIZE // 2
    freqs = jnp.exp(jnp.arange(half, dtype=F32) * (-2.0 * math.log(ROPE_BASE) / HEAD_SIZE))
    order = jnp.transpose(freqs.reshape(8, 8), (1, 0)).reshape(half)
    angle = order[:, None] * positions[None, :]
    return jnp.cos(angle), jnp.sin(angle)


def on_device(
    counts, layer_input, gain, codes, column_scale_quantized, block_second_scale,
    query_down_map, query_up_map, token_document, output_cotangent,
):
    ctx_count, fsdp_count = counts
    total = ctx_count * fsdp_count
    chips = ctx_count // 2
    rows, width = layer_input.shape
    tokens = 2 * rows
    cos_t, sin_t = rope_tables(lax.axis_index("ctx") // 2, tokens)
    vm = pl.BlockSpec(memory_space=pltpu.VMEM)
    blocks = column_scale_quantized.shape[0]
    rank, local_columns = query_up_map.shape
    heads = local_columns // HEAD_SIZE // 2
    ga_owners = math.gcd(total, width // 128)
    up_pieces = 2 * heads
    vmem, dma = pltpu.VMEM, pltpu.SemaphoreType.DMA
    attn, ga, up = pl.pallas_call(
        functools.partial(step_kernel, counts),
        out_shape=(
            jax.ShapeDtypeStruct(output_cotangent.shape, BF16),
            jax.ShapeDtypeStruct((rank, width), F32),
            jax.ShapeDtypeStruct(query_up_map.shape, F32),
        ),
        in_specs=[vm] * 11,
        out_specs=(vm,) * 3,
        scratch_shapes=[
            vmem((24, blocks, 128), F32),
            vmem((8, blocks // 2, 128), F32),
            vmem((2, tokens, 1024), F32),
            vmem((8, 128, tokens), F32),
            vmem((tokens, width), BF16),
            vmem((8, 32, tokens), F32),
            vmem((8, 32, tokens), BF16),
            vmem((8, 32, tokens), BF16),
            vmem((8, 16 * heads, tokens), F32),
            vmem((8, 16 * heads, tokens), BF16),
            vmem((8, 16 * heads, tokens), BF16),
            vmem((tokens, heads * 128), BF16),
            vmem((16, tokens), BF16),
            vmem((chips, tokens + 16, 256), BF16),
            vmem((256, heads * tokens), BF16),
            vmem((128, heads * tokens), BF16),
            vmem((256 + 16, tokens), BF16),
            vmem((8 * heads, tokens), F32),
            vmem((heads, 256 + 16, tokens), F32),
            vmem((heads, 128 + 16, tokens), F32),
            vmem((8, 128), F32),
            vmem((tokens, heads * 128), BF16),
            vmem((rows, heads * 128), BF16),
            vmem((ga_owners, rank, 128), BF16),
            vmem((total, rank, 128), BF16),
            vmem((rank, 128), BF16),
            vmem((ga_owners, rank, 128), BF16),
            vmem((up_pieces, 8, 128), F32),
            vmem((chips, 8, 128), F32),
            vmem((8, 128), F32),
            vmem((2 * up_pieces, 8, 128), F32),
            dma((6,)),
            dma((6,)),
            dma((1,)),
            dma((chips,)),
            dma((8,)),
        ],
        compiler_params=pltpu.CompilerParams(
            collective_id=0, has_side_effects=True, vmem_limit_bytes=60 * 1024 * 1024
        ),
        name="step",
    )(
        layer_input, gain[None, :], codes, column_scale_quantized, block_second_scale[:, None],
        query_down_map.T, query_up_map, token_document[None, :], cos_t, sin_t, output_cotangent,
    )
    return attn, ga.T, up


def solution(mesh):
    return jax.shard_map(
        functools.partial(on_device, (mesh.shape["ctx"], mesh.shape["fsdp"])),
        mesh=mesh,
        in_specs=(
            P("ctx", None),
            P(),
            P("fsdp", None),
            P("fsdp", None),
            P(),
            P(),
            P(None, "fsdp"),
            P("ctx"),
            P("ctx", "fsdp"),
        ),
        out_specs=(P("ctx", "fsdp"), P(), P(None, "fsdp")),
        check_vma=False,
    )
```

```python
import math
import functools

import jax
import jax.numpy as jnp
from jax import lax
from jax.experimental import pallas as pl
from jax.experimental.pallas import tpu as pltpu
from jax.sharding import PartitionSpec as P

HEAD_SIZE = 128
ADAPTER_SCALE = 2.0
ROPE_BASE = 500000.0
MESH = pl.DeviceIdType.MESH
F32 = jnp.float32
BF16 = jnp.bfloat16
I16 = jnp.int16

NF4_LEVELS = [
    -1.0,
    -0.6961928009986877,
    -0.5250730514526367,
    -0.39491748809814453,
    -0.28444138169288635,
    -0.18477343022823334,
    -0.09105003625154495,
    0.0,
    0.07958029955625534,
    0.16093020141124725,
    0.24611230194568634,
    0.33791524171829224,
    0.44070982933044434,
    0.5626170039176941,
    0.7229568362236023,
    1.0,
]


def take_lanes(values, index):
    return jnp.take_along_axis(values, index, axis=1, mode="promise_in_bounds")


GATHERED = (1, 3, 5, 7)
LANE_PICK = lax.GatherDimensionNumbers(
    offset_dims=(), collapsed_slice_dims=(1,), start_index_map=(1,),
    operand_batching_dims=(0,), start_indices_batching_dims=(0,),
)


def pick_lanes(values, index):
    return lax.gather(
        values, index[..., None], LANE_PICK, (1, 1),
        mode=lax.GatherScatterMode.PROMISE_IN_BOUNDS,
    )


def dot(a, b):
    return jnp.dot(a, b, preferred_element_type=F32)


def nt(a, b):
    return lax.dot_general(a, b, (((1,), (1,)), ((), ())), preferred_element_type=F32)


def tn(a, b):
    return lax.dot_general(a, b, (((0,), (0,)), ((), ())), preferred_element_type=F32)


def eye(size):
    row = lax.broadcasted_iota(jnp.int32, (size, size), 0)
    col = lax.broadcasted_iota(jnp.int32, (size, size), 1)
    return (row == col).astype(F32).astype(BF16)


def step_kernel(
    counts,
    x_hbm, gain_hbm, codes_hbm, cs_hbm, bss_hbm, qdown_hbm, qup_hbm, ids_hbm, do_hbm,
    out_ref, ga_out, up_out,
    x_ref, gain_ref, codes_ref, cs_ref, bss_ref, qdown_ref, qup_ref, ids_ref, do_ref, scl, vscl, acc, acct, xn, cos_ref, sin_ref, own_kv, send_kv, recv_kv, own_q, send_q, recv_q,
    do_all, ids_own, ids_all, kv_all, queries, cotans, vk, row_max, out_acc, grad_acc, lin,
    out_stage, out_in, mid_own, mid_in,
    ga_part, ga_in, ga_sum, ga_all, up_part, up_in, up_sum, up_all,
    load, pair_send, pair_recv, block_send, block_recv, sems,
):
    loads = [
        pltpu.make_async_copy(src, dst, load.at[number])
        for number, (src, dst) in enumerate(
            (
                (x_hbm, x_ref), (gain_hbm, gain_ref), (ids_hbm, ids_ref), (do_hbm, do_ref),
                (bss_hbm, bss_ref), (cs_hbm, cs_ref), (codes_hbm, codes_ref),
                (qdown_hbm, qdown_ref), (qup_hbm, qup_ref),
            )
        )
    ]
    for copy in loads:
        copy.start()
    ctx_count, fsdp_count = counts
    total = ctx_count * fsdp_count
    ctx, member = lax.axis_index("ctx"), lax.axis_index("fsdp")
    me = ctx * fsdp_count + member
    partner = 1 - member
    chip, core = ctx // 2, lax.rem(ctx, 2)
    outer, inner = chip // 2, lax.rem(chip, 2)
    sibling = ctx + 1 - 2 * core
    chips = ctx_count // 2
    rows, width = x_ref.shape
    tokens = 2 * rows
    depth = codes_ref.shape[0]
    half_depth = depth // 2
    blocks = cs_ref.shape[0]
    block_rows = depth // blocks
    half_blocks = blocks // 2

    barrier = pltpu.get_barrier_semaphore()

    def greet(step, carry):
        other = lax.rem(me + step, total)
        pl.semaphore_signal(
            barrier, inc=1, device_id=(other // fsdp_count, lax.rem(other, fsdp_count)),
            device_id_type=MESH,
        )
        return carry

    lax.fori_loop(1, total, greet, 0)

    mine_at = pl.multiple_of(core * rows, rows)
    other_at = pl.multiple_of((1 - core) * rows, rows)
    for copy in loads[:3]:
        copy.wait()
    for r in range(0, rows, 16):
        wide = x_ref[r : r + 16, :].astype(F32)
        inverse = lax.rsqrt(jnp.mean(wide * wide, axis=-1, keepdims=True) + 1e-05)
        xn[pl.ds(pl.multiple_of(mine_at + r, 16), 16), :] = (
            wide * inverse * gain_ref[...]
        ).astype(BF16)
    ids_own[...] = jnp.broadcast_to(
        ids_ref[...].astype(F32), (16, rows)
    ).astype(BF16)
    half_columns = do_ref.shape[1] // 2
    mine_columns = pl.multiple_of(core * half_columns, 128)
    other_columns = pl.multiple_of((1 - core) * half_columns, 128)
    loads[3].wait()
    do_all[pl.ds(mine_at, rows), :] = do_ref[:, pl.ds(mine_columns, half_columns)]

    pl.semaphore_wait(barrier, total - 1)

    def pair_copy(src, dst, number, device):
        copy = pltpu.make_async_remote_copy(
            src_ref=src, dst_ref=dst, send_sem=pair_send.at[number],
            recv_sem=pair_recv.at[number], device_id=device, device_id_type=MESH,
        )
        copy.start()
        return copy

    across = (sibling, member)
    beside = (ctx, partner)
    span = pl.ds(mine_at, rows)
    copy_x = pair_copy(xn.at[span], xn.at[span], 0, across)
    copy_do = pair_copy(
        do_ref.at[:, pl.ds(other_columns, half_columns)], do_all.at[span], 2, across
    )

    def send(src, dst, number, ctx_to, fsdp_to):
        pltpu.make_async_remote_copy(
            src_ref=src, dst_ref=dst, send_sem=sems.at[2 * number],
            recv_sem=sems.at[2 * number + 1], device_id=(ctx_to, fsdp_to),
            device_id_type=MESH,
        ).start()

    def hold(src, dst, number):
        pltpu.make_async_copy(src, dst, sems.at[2 * number + 1]).start()

    def await_all(buffer, number):
        pltpu.make_async_copy(buffer, buffer, sems.at[2 * number + 1]).wait()

    def tell_ids(step, carry):
        send(ids_own, ids_all.at[chip, :, span], 4, lax.rem(ctx + step, ctx_count), member)
        return carry

    lax.fori_loop(1, ctx_count, tell_ids, 0)

    lane = lax.broadcasted_iota(jnp.int32, (blocks, 128), 1)
    loads[4].wait()
    loads[5].wait()
    all_blocks = bss_ref.shape[1]
    scale_row = lax.broadcasted_iota(jnp.int32, (blocks, all_blocks), 0) + member * blocks
    scale_lane = lax.broadcasted_iota(jnp.int32, (blocks, all_blocks), 1)
    second = jnp.sum(
        jnp.where(scale_row == scale_lane, bss_ref[...], 0.0), axis=1, keepdims=True
    )
    for tile in range(3):
        source = [
            (cs_ref[:, tile * 1024 + m * 128 : tile * 1024 + (m + 1) * 128].astype(F32) + 1.0)
            / 256.0
            * second
            for m in range(8)
        ]
        for n in range(8):
            index = 8 * (lane % 16) + n
            picked = take_lanes(source[0], index)
            for m in range(1, 8):
                picked = jnp.where(lane // 16 == m, take_lanes(source[m], index), picked)
            scl[tile * 8 + n] = picked

    at = lax.broadcasted_iota(jnp.int32, (64, tokens), 0)
    feature = (8 * (at % 8) + at // 8).astype(F32)
    position = (lax.broadcasted_iota(jnp.int32, (64, tokens), 1) + chip * tokens).astype(F32)
    angle = position * jnp.exp(feature * (-2.0 * math.log(ROPE_BASE) / HEAD_SIZE))
    cos_ref[...] = jnp.cos(angle)
    sin_ref[...] = jnp.sin(angle)

    pr = lax.broadcasted_iota(jnp.int32, (128, 128), 0)
    pd = lax.broadcasted_iota(jnp.int32, (128, 128), 1)
    perm = (pd == 8 * (pr % 16) + pr // 16).astype(F32).astype(BF16)
    eye_wide = eye(256)

    chunk = 512
    per_chunk = chunk // block_rows
    short_lane = lax.broadcasted_iota(jnp.int32, (block_rows, 128), 1)
    half_lane = lax.broadcasted_iota(jnp.int32, (half_blocks, 128), 1)
    long_lane = lax.broadcasted_iota(jnp.int32, (tokens, 128), 1)
    levels = [jnp.full((block_rows, 128), level, BF16) for level in NF4_LEVELS]
    table = jnp.zeros((block_rows, 128), F32)
    for code, level in enumerate(NF4_LEVELS):
        table = jnp.where(short_lane % 16 == code, F32(level), table)

    def phase(paired, tile, half):
        if paired:
            shift = 16 + 96 * core

            def chosen(lanes):
                return lax.rem(lanes // 16, 2) == core

            def words_at(at):
                return jnp.where(
                    short_lane < 64,
                    codes_ref[pl.ds(at, block_rows), 128:256],
                    codes_ref[pl.ds(at, block_rows), 256:384],
                )
        else:
            shift = 64
            tile_at = pl.multiple_of(tile * 128, 128)

            def chosen(lanes):
                return lanes // 64 == half

            def words_at(at):
                return codes_ref[pl.ds(at, block_rows), pl.ds(tile_at, 128)]

        for n in range(8):
            if paired:
                scale = jnp.where(lane < 64, scl[8 + n], scl[16 + n])
            else:
                scale = scl[tile * 8 + n]
            vscl[n] = jnp.where(
                chosen(half_lane), scale[:half_blocks], pltpu.roll(scale[half_blocks:], shift, 1)
            )
        acc[...] = jnp.zeros_like(acc)
        first = chosen(short_lane)

        def step(k, carry):
            at = pl.multiple_of(member * depth + k * chunk, 128)
            lower = xn[:, pl.ds(at, chunk)]
            upper = xn[:, pl.ds(pl.multiple_of(at + half_depth, 128), chunk)]
            low_words, high_words, full_words = [], [], []
            for b in range(per_chunk):
                row = pl.multiple_of(k * chunk + b * block_rows, block_rows)
                words = jnp.where(
                    first,
                    words_at(row),
                    pltpu.roll(words_at(pl.multiple_of(row + half_depth, block_rows)), shift, 1),
                )
                full_words.append(words)
                low_words.append(words.astype(I16))
                high_words.append(jnp.right_shift(words, 16).astype(I16))
            for pair in range(4):
                planes = []
                for n in (2 * pair, 2 * pair + 1):
                    pieces = []
                    for b in range(per_chunk):
                        scale = vscl[n, pl.ds(k * per_chunk + b, 1), :]
                        if n % 8 in GATHERED:
                            code = jnp.bitwise_and(jnp.right_shift(full_words[b], 4 * n), 15)
                            pieces.append((pick_lanes(table, code) * scale).astype(BF16))
                            continue
                        words = low_words[b] if n < 4 else high_words[b]
                        values = levels
                        for bit in range(4):
                            place = 4 * (n % 4) + bit
                            mark = 1 << place if place < 15 else -(1 << 15)
                            mask = (words & jnp.int16(mark)) != 0
                            values = [
                                jnp.where(mask, values[v + 1], values[v])
                                for v in range(0, len(values), 2)
                            ]
                        pieces.append(values[0] * scale.astype(BF16))
                    planes.append(jnp.concatenate(pieces, axis=0))
                weight = jnp.concatenate(planes, axis=1)
                columns = slice(pair * 256, (pair + 1) * 256)
                acc[0, :, columns] += dot(lower, weight)
                acc[1, :, columns] += dot(upper, weight)
            return carry

        lax.fori_loop(0, half_depth // chunk, step, 0)
        keep = chosen(long_lane)
        for n in range(8):
            columns = slice(n * 128, (n + 1) * 128)
            acct[n] = jnp.where(keep, acc[0, :, columns], acc[1, :, columns]).T

    loads[6].wait()
    copy_x.wait()

    def kv_field(group, part):
        at = pl.multiple_of(64 * group, 64) + 32 * part
        return acct[:, pl.ds(pl.multiple_of(at, 32), 16), :] + acct[
            :, pl.ds(pl.multiple_of(at + 16, 16), 16), :
        ]

    phase(True, 0, 0)
    for part in range(2):
        send_kv[:, 16 * part : 16 * part + 16, :] = kv_field(partner, part).astype(BF16)
    copy_kv = pair_copy(send_kv, recv_kv, 3, beside)
    for part in range(2):
        own_kv[:, 16 * part : 16 * part + 16, :] = kv_field(member, part)

    place = 3 * partner + core
    phase(False, place // 2, lax.rem(place, 2))
    send_q[...] = (acct[:, :64, :] + acct[:, 64:, :]).astype(BF16)
    copy_q = pair_copy(send_q, recv_q, 4, beside)

    loads[7].wait()
    loads[8].wait()
    lr_t = nt(qdown_ref[...], xn[...]).astype(BF16)
    copy_do.wait()
    hold(ids_own, ids_all.at[chip, :, span], 4)
    await_all(ids_all, 4)
    my_ids = ids_all[chip]
    heads = own_q.shape[1] // 16
    local = pl.multiple_of(core * heads * 128, 128)
    marks = lax.broadcasted_iota(jnp.int32, (128, tokens), 0).astype(F32)
    tags = (marks == jnp.broadcast_to(my_ids[:1].astype(F32), (128, tokens))).astype(F32)
    tags = tags.astype(BF16)
    for head in range(heads):
        columns = slice(head * tokens, (head + 1) * tokens)
        queries[128:, columns] = tags
        cotans[:, columns] = nt(perm, do_all[:, head * 128 : (head + 1) * 128]).astype(BF16)

    cosine = cos_ref[...].reshape(8, 8, tokens)
    sine = sin_ref[...].reshape(8, 8, tokens)

    def rotate(field):
        a, b = field[:, :8, :], field[:, 8:, :]
        return jnp.concatenate([a * cosine - b * sine, b * cosine + a * sine], axis=1)

    copy_kv.wait()
    key = own_kv[:, :16, :] + recv_kv[:, :16, :].astype(F32)
    value = own_kv[:, 16:, :] + recv_kv[:, 16:, :].astype(F32)
    fields = jnp.concatenate(
        [value.reshape(128, tokens).astype(BF16), rotate(key).reshape(128, tokens).astype(BF16)],
        axis=0,
    )
    kv_all[chip] = tn(fields, eye_wide).astype(BF16)

    def send_block(block, to_chip):
        pltpu.make_async_remote_copy(
            src_ref=kv_all.at[block], dst_ref=kv_all.at[block],
            send_sem=block_send.at[0], recv_sem=block_recv.at[block],
            device_id=(2 * to_chip + core, member), device_id_type=MESH,
        ).start()

    def await_block(block):
        pltpu.make_async_copy(kv_all.at[block], kv_all.at[block], block_recv.at[block]).wait()

    @pl.when(inner == 0)
    def _():
        send_block(chip, chip + 1)

    def along(step, carry):
        send_block(chip, chip + 2 * step)
        return carry

    lax.fori_loop(1, chips // 2 - outer, along, 0)

    place = 3 * member + core
    phase(False, place // 2, lax.rem(place, 2))
    own_q[...] = acct[:, :64, :] + acct[:, 64:, :]

    copy_q.wait()
    for head in range(heads):
        columns = slice(head * tokens, (head + 1) * tokens)
        up_cols = qup_ref[:, pl.ds(pl.multiple_of(local + head * 128, 128), 128)]
        adapter = dot(nt(perm, up_cols).astype(BF16), lr_t).reshape(8, 16, tokens)
        query = own_q[:, 16 * head : 16 * head + 16, :]
        query = query + recv_q[:, 16 * head : 16 * head + 16, :].astype(F32)
        query = query + ADAPTER_SCALE * adapter
        queries[:128, columns] = rotate(query).reshape(128, tokens).astype(BF16)

    soft_scale = 1.0 / math.sqrt(HEAD_SIZE)
    log_scale = soft_scale / math.log(2.0)
    tag_row = lax.broadcasted_iota(jnp.int32, (16, tokens), 0).astype(F32)
    spread_row = lax.broadcasted_iota(jnp.int32, (16, 128), 0)
    spread_lane = lax.broadcasted_iota(jnp.int32, (16, 128), 1)
    spread_tags = (spread_row == spread_lane).astype(F32).astype(BF16)
    vk[256:, :] = jnp.ones((16, tokens), BF16)

    def attend(block, diagonal):
        both = kv_all[block]
        block_ids = ids_all[block].astype(F32)
        barred = jnp.where(block_ids == tag_row, 0.0, -1e30).astype(BF16)
        barred = tn(barred, spread_tags).astype(BF16)
        lhs = jnp.concatenate([both[:, 128:], barred], axis=1)
        vk[:256, :] = nt(eye_wide, both).astype(BF16)
        for head in range(heads):
            columns = slice(head * tokens, (head + 1) * tokens)
            row = slice(8 * head, 8 * head + 1)
            scores = dot(lhs, queries[:, columns]) * log_scale
            if diagonal:
                ki = lax.broadcasted_iota(jnp.int32, (tokens, tokens), 0)
                qi = lax.broadcasted_iota(jnp.int32, (tokens, tokens), 1)
                scores = jnp.where(ki <= qi, scores, -1e30)
            top = jnp.max(scores, axis=0, keepdims=True)
            if not diagonal:
                before = row_max[row, :]
                top = jnp.maximum(top, before)
            expo = jnp.exp2(scores - top)
            weighted = expo * dot(both[:, :128], cotans[:, columns])
            new_out = dot(vk[...], expo.astype(BF16))
            new_grad = dot(vk[128:, :], weighted.astype(BF16))
            row_max[row, :] = top
            if diagonal:
                out_acc[head] = new_out
                grad_acc[head] = new_grad
            else:
                decay = jnp.exp2(before - top)
                out_acc[head] = decay * out_acc[head] + new_out
                grad_acc[head] = decay * grad_acc[head] + new_grad

    attend(chip, True)

    def visit(step, carry):
        place = step - inner
        odd = lax.rem(place + 2, 2) == 1
        ahead = (place + 1) // 2

        @pl.when(((step == 0) | odd) & (ahead < outer))
        def _():
            block = 2 * (outer - 1 - ahead) + inner
            await_block(block)
            send_block(block, 2 * outer + 1 - inner)

        crossed = 2 * (outer - 1 - (place - 1) // 2) + 1 - inner
        crossed = jnp.where(place < 0, chip - 1, crossed)
        column = 2 * (outer - 1 - place // 2) + inner
        block = jnp.where(odd, crossed, column)

        @pl.when(odd)
        def _():
            await_block(block)

        attend(block, False)
        return carry

    lax.fori_loop(0, chip, visit, 0)

    middle = jnp.zeros((16, tokens), F32)
    for head in range(heads):
        inverse = 1.0 / out_acc[head, 256:257, :]
        mean_dot = grad_acc[head, 128:129, :] * inverse
        grad = grad_acc[head, :128, :] - mean_dot * out_acc[head, 128:256, :]
        grad = (soft_scale * inverse * grad).reshape(8, 16, tokens)
        a, b = grad[:, :8, :], grad[:, 8:, :]
        turned = jnp.concatenate([a * cosine + b * sine, b * cosine - a * sine], axis=1)
        lin_t = turned.reshape(128, tokens).astype(BF16)
        lin[head] = lin_t
        up_cols = qup_ref[:, pl.ds(pl.multiple_of(local + head * 128, 128), 128)]
        middle = middle + dot(nt(up_cols, perm).astype(BF16), lin_t)
    mid_own[...] = middle
    quarter = 2 * core + member
    mid_copies = [
        pair_copy(mid_own, mid_in.at[number], 6 + number, device)
        for number, device in enumerate(((ctx, partner), (sibling, partner), (sibling, member)))
    ]

    up_pieces = up_part.shape[0]
    up_stride = chips // up_pieces
    up_mine = chip // up_stride
    owner = lax.rem(chip, up_stride) == 0
    up_slot = core * up_pieces + up_mine
    ga_slot = quarter * up_pieces + up_mine
    low = chip < chips // 2

    def far_first(step, count):
        return jnp.where(low, count - 1 - step, step)

    back = 16 * (pd % 8) + pd // 8
    for head in range(heads):
        up = take_lanes(ADAPTER_SCALE * nt(lr_t, lin[head]), back[:16])
        up_part[2 * head] = up[:8]
        up_part[2 * head + 1] = up[8:]

    def scatter(part, into, number):
        def one(step, carry):
            j = far_first(step, up_pieces)
            to = j * up_stride

            @pl.when(to != chip)
            def _():
                send(part.at[j], into.at[chip], number, 2 * to + core, member)

            return carry

        lax.fori_loop(0, up_pieces, one, 0)

        @pl.when(owner)
        def _():
            hold(part.at[up_mine], into.at[chip], number)

    scatter(up_part, up_in, 0)

    for head in range(heads):
        inverse = 1.0 / out_acc[head, 256:257, :]
        out = (out_acc[head, :128, :] * inverse).astype(BF16)
        out_stage[:, head * 128 : (head + 1) * 128] = tn(out, perm).astype(BF16)

    for copy in mid_copies:
        copy.wait()
    middle = mid_own[...] + mid_in[0] + mid_in[1] + mid_in[2]
    middle = (ADAPTER_SCALE * middle).astype(BF16)
    share = up_pieces * 128
    ga = dot(middle, xn[:, pl.ds(pl.multiple_of(quarter * share, 128), share)])
    for j in range(up_pieces):
        ga_part[j] = ga[:, j * 128 : (j + 1) * 128].astype(BF16)
    scatter(ga_part, ga_in, 1)

    copy_out = pair_copy(out_stage.at[pl.ds(other_at, rows)], out_in, 5, across)
    out_ref[:, pl.ds(mine_columns, half_columns)] = out_stage[pl.ds(mine_at, rows), :]

    @pl.when(owner)
    def _():
        await_all(up_in, 0)
        up_sum[...] = jnp.sum(up_in[...], axis=0)

        def spread_up(step, carry):
            to = far_first(step, ctx_count)

            @pl.when(to != ctx)
            def _():
                send(up_sum, up_all.at[up_slot], 2, to, member)

            return carry

        lax.fori_loop(0, ctx_count, spread_up, 0)
        hold(up_sum, up_all.at[up_slot], 2)

        await_all(ga_in, 1)
        ga_sum[...] = jnp.sum(ga_in[...].astype(F32), axis=0).astype(BF16)

        def spread_ga(step, carry):
            place = far_first(step, total)
            to, to_fsdp = place // fsdp_count, lax.rem(place, fsdp_count)

            @pl.when(place != me)
            def _():
                send(ga_sum, ga_all.at[ga_slot], 3, to, to_fsdp)

            return carry

        lax.fori_loop(0, total, spread_ga, 0)
        hold(ga_sum, ga_all.at[ga_slot], 3)

    copy_out.wait()
    out_ref[:, pl.ds(other_columns, half_columns)] = out_in[...]

    await_all(up_all, 2)
    for j in range(2 * up_pieces):
        row, col = 8 * (j % 2), 128 * (j // 2)
        up_out[row : row + 8, col : col + 128] = up_all[j]
    await_all(ga_all, 3)
    for j in range(4 * up_pieces):
        ga_out[:, j * 128 : (j + 1) * 128] = ga_all[j].astype(F32)

    def drain(buffer, semaphore, sent):
        def one(step, carry):
            pltpu.make_async_copy(buffer, buffer, semaphore).wait()
            return carry

        lax.fori_loop(0, sent, one, 0)

    passed = chips // 2 - 1 - outer + outer + 1 - inner
    drain(kv_all.at[chip], block_send.at[0], passed)
    scattered = up_pieces - owner.astype(jnp.int32)
    drain(up_part.at[0], sems.at[0], scattered)
    drain(ga_part.at[0], sems.at[2], scattered)
    drain(up_sum, sems.at[4], jnp.where(owner, ctx_count - 1, 0))
    drain(ga_sum, sems.at[6], jnp.where(owner, total - 1, 0))
    drain(ids_own, sems.at[8], ctx_count - 1)


def on_device(
    counts, layer_input, gain, codes, column_scale_quantized, block_second_scale,
    query_down_map, query_up_map, token_document, output_cotangent,
):
    ctx_count, fsdp_count = counts
    total = ctx_count * fsdp_count
    chips = ctx_count // 2
    rows, width = layer_input.shape
    tokens = 2 * rows
    vm = pl.BlockSpec(memory_space=pltpu.VMEM)
    hbm = pl.BlockSpec(memory_space=pltpu.HBM)
    blocks = column_scale_quantized.shape[0]
    rank, local_columns = query_up_map.shape
    heads = local_columns // HEAD_SIZE // 2
    up_pieces = 2 * heads
    vmem, dma = pltpu.VMEM, pltpu.SemaphoreType.DMA
    attn, ga, up = pl.pallas_call(
        functools.partial(step_kernel, counts),
        out_shape=(
            vmem(output_cotangent.shape, BF16),
            vmem((rank, width), F32),
            vmem(query_up_map.shape, F32),
        ),
        in_specs=[hbm] * 9,
        out_specs=(vm,) * 3,
        scratch_shapes=[
            vmem(layer_input.shape, BF16),
            vmem((1, width), F32),
            vmem(codes.shape, jnp.int32),
            vmem(column_scale_quantized.shape, jnp.int32),
            vmem((1, block_second_scale.shape[0]), F32),
            vmem((rank, width), BF16),
            vmem(query_up_map.shape, BF16),
            vmem((1, rows), jnp.int32),
            vmem(output_cotangent.shape, BF16),
            vmem((24, blocks, 128), F32),
            vmem((8, blocks // 2, 128), F32),
            vmem((2, tokens, 1024), F32),
            vmem((8, 128, tokens), F32),
            vmem((tokens, width), BF16),
            vmem((HEAD_SIZE // 2, tokens), F32),
            vmem((HEAD_SIZE // 2, tokens), F32),
            vmem((8, 32, tokens), F32),
            vmem((8, 32, tokens), BF16),
            vmem((8, 32, tokens), BF16),
            vmem((8, 16 * heads, tokens), F32),
            vmem((8, 16 * heads, tokens), BF16),
            vmem((8, 16 * heads, tokens), BF16),
            vmem((tokens, heads * 128), BF16),
            vmem((16, rows), BF16),
            vmem((chips, 16, tokens), BF16),
            vmem((chips, tokens, 256), BF16),
            vmem((256, heads * tokens), BF16),
            vmem((128, heads * tokens), BF16),
            vmem((256 + 16, tokens), BF16),
            vmem((8 * heads, tokens), F32),
            vmem((heads, 256 + 16, tokens), F32),
            vmem((heads, 128 + 16, tokens), F32),
            vmem((heads, 128, tokens), BF16),
            vmem((tokens, heads * 128), BF16),
            vmem((rows, heads * 128), BF16),
            vmem((rank, tokens), F32),
            vmem((3, rank, tokens), F32),
            vmem((up_pieces, rank, 128), BF16),
            vmem((chips, rank, 128), BF16),
            vmem((rank, 128), BF16),
            vmem((4 * up_pieces, rank, 128), BF16),
            vmem((up_pieces, 8, 128), F32),
            vmem((chips, 8, 128), F32),
            vmem((8, 128), F32),
            vmem((2 * up_pieces, 8, 128), F32),
            dma((9,)),
            dma((9,)),
            dma((9,)),
            dma((1,)),
            dma((chips,)),
            dma((10,)),
        ],
        compiler_params=pltpu.CompilerParams(
            collective_id=0, has_side_effects=True, vmem_limit_bytes=56 * 1024 * 1024
        ),
        name="step",
    )(
        layer_input, gain[None, :], codes, column_scale_quantized, block_second_scale[None, :],
        query_down_map.T, query_up_map, token_document[None, :], output_cotangent,
    )
    return attn, ga.T, up


def solution(mesh):
    return jax.shard_map(
        functools.partial(on_device, (mesh.shape["ctx"], mesh.shape["fsdp"])),
        mesh=mesh,
        in_specs=(
            P("ctx", None),
            P(),
            P("fsdp", None),
            P("fsdp", None),
            P(),
            P(),
            P(None, "fsdp"),
            P("ctx"),
            P("ctx", "fsdp"),
        ),
        out_specs=(P("ctx", "fsdp"), P(), P(None, "fsdp")),
        check_vma=False,
    )
```

```python
import math
import functools

import jax
import jax.numpy as jnp
from jax import lax
from jax.experimental import pallas as pl
from jax.experimental.pallas import tpu as pltpu
from jax.sharding import PartitionSpec as P

HEAD_SIZE = 128
ADAPTER_SCALE = 2.0
ROPE_BASE = 500000.0
MESH = pl.DeviceIdType.MESH
F32 = jnp.float32
BF16 = jnp.bfloat16
I16 = jnp.int16

NF4_LEVELS = [
    -1.0,
    -0.6961928009986877,
    -0.5250730514526367,
    -0.39491748809814453,
    -0.28444138169288635,
    -0.18477343022823334,
    -0.09105003625154495,
    0.0,
    0.07958029955625534,
    0.16093020141124725,
    0.24611230194568634,
    0.33791524171829224,
    0.44070982933044434,
    0.5626170039176941,
    0.7229568362236023,
    1.0,
]


def take_lanes(values, index):
    return jnp.take_along_axis(values, index, axis=1, mode="promise_in_bounds")


GATHERED = (1, 3, 5, 7)
LANE_PICK = lax.GatherDimensionNumbers(
    offset_dims=(), collapsed_slice_dims=(1,), start_index_map=(1,),
    operand_batching_dims=(0,), start_indices_batching_dims=(0,),
)


def pick_lanes(values, index):
    return lax.gather(
        values, index[..., None], LANE_PICK, (1, 1),
        mode=lax.GatherScatterMode.PROMISE_IN_BOUNDS,
    )


def dot(a, b):
    return jnp.dot(a, b, preferred_element_type=F32)


def nt(a, b):
    return lax.dot_general(a, b, (((1,), (1,)), ((), ())), preferred_element_type=F32)


def tn(a, b):
    return lax.dot_general(a, b, (((0,), (0,)), ((), ())), preferred_element_type=F32)


def eye(size):
    row = lax.broadcasted_iota(jnp.int32, (size, size), 0)
    col = lax.broadcasted_iota(jnp.int32, (size, size), 1)
    return (row == col).astype(F32).astype(BF16)


def step_kernel(
    counts,
    x_hbm, gain_hbm, codes_hbm, cs_hbm, bss_hbm, qdown_hbm, qup_hbm, ids_hbm, do_hbm,
    out_ref, ga_out, up_out,
    x_ref, gain_ref, codes_ref, cs_ref, bss_ref, qdown_ref, qup_ref, ids_ref, do_ref, scl, vscl, acc, acct, xn, cos_ref, sin_ref, own_kv, send_kv, recv_kv, own_q, send_q, recv_q,
    do_all, ids_own, ids_all, kv_all, queries, cotans, vk, row_max, out_acc, grad_acc, lin,
    score_buf, dots_buf, prob_buf, weight_buf, out_stage, out_in, mid_own, mid_in,
    ga_part, ga_in, ga_sum, ga_all, up_part, up_in, up_sum, up_all,
    load, pair_send, pair_recv, block_send, block_recv, sems,
):
    loads = [
        pltpu.make_async_copy(src, dst, load.at[number])
        for number, (src, dst) in enumerate(
            (
                (x_hbm, x_ref), (gain_hbm, gain_ref), (ids_hbm, ids_ref), (do_hbm, do_ref),
                (bss_hbm, bss_ref), (cs_hbm, cs_ref), (codes_hbm, codes_ref),
                (qdown_hbm, qdown_ref), (qup_hbm, qup_ref),
            )
        )
    ]
    for copy in loads:
        copy.start()
    ctx_count, fsdp_count = counts
    total = ctx_count * fsdp_count
    ctx, member = lax.axis_index("ctx"), lax.axis_index("fsdp")
    me = ctx * fsdp_count + member
    partner = 1 - member
    chip, core = ctx // 2, lax.rem(ctx, 2)
    outer, inner = chip // 2, lax.rem(chip, 2)
    sibling = ctx + 1 - 2 * core
    chips = ctx_count // 2
    rows, width = x_ref.shape
    tokens = 2 * rows
    depth = codes_ref.shape[0]
    half_depth = depth // 2
    blocks = cs_ref.shape[0]
    block_rows = depth // blocks
    half_blocks = blocks // 2

    barrier = pltpu.get_barrier_semaphore()

    def greet(step, carry):
        other = lax.rem(me + step, total)
        pl.semaphore_signal(
            barrier, inc=1, device_id=(other // fsdp_count, lax.rem(other, fsdp_count)),
            device_id_type=MESH,
        )
        return carry

    lax.fori_loop(1, total, greet, 0)

    mine_at = pl.multiple_of(core * rows, rows)
    other_at = pl.multiple_of((1 - core) * rows, rows)
    for copy in loads[:3]:
        copy.wait()
    for r in range(0, rows, 16):
        wide = x_ref[r : r + 16, :].astype(F32)
        inverse = lax.rsqrt(jnp.mean(wide * wide, axis=-1, keepdims=True) + 1e-05)
        xn[pl.ds(pl.multiple_of(mine_at + r, 16), 16), :] = (
            wide * inverse * gain_ref[...]
        ).astype(BF16)
    ids_own[...] = jnp.broadcast_to(
        ids_ref[...].astype(F32), (16, rows)
    ).astype(BF16)
    half_columns = do_ref.shape[1] // 2
    mine_columns = pl.multiple_of(core * half_columns, 128)
    other_columns = pl.multiple_of((1 - core) * half_columns, 128)
    loads[3].wait()
    do_all[pl.ds(mine_at, rows), :] = do_ref[:, pl.ds(mine_columns, half_columns)]

    pl.semaphore_wait(barrier, total - 1)

    def pair_copy(src, dst, number, device):
        copy = pltpu.make_async_remote_copy(
            src_ref=src, dst_ref=dst, send_sem=pair_send.at[number],
            recv_sem=pair_recv.at[number], device_id=device, device_id_type=MESH,
        )
        copy.start()
        return copy

    across = (sibling, member)
    beside = (ctx, partner)
    span = pl.ds(mine_at, rows)
    near = xn.at[span, pl.ds(pl.multiple_of(member * depth, 128), depth)]
    far = xn.at[span, pl.ds(pl.multiple_of(partner * depth, 128), depth)]
    copy_x = pair_copy(near, near, 0, across)
    copy_x_rest = pair_copy(far, far, 1, across)
    copy_do = pair_copy(
        do_ref.at[:, pl.ds(other_columns, half_columns)], do_all.at[span], 2, across
    )

    def send(src, dst, number, ctx_to, fsdp_to):
        pltpu.make_async_remote_copy(
            src_ref=src, dst_ref=dst, send_sem=sems.at[2 * number],
            recv_sem=sems.at[2 * number + 1], device_id=(ctx_to, fsdp_to),
            device_id_type=MESH,
        ).start()

    def hold(src, dst, number):
        pltpu.make_async_copy(src, dst, sems.at[2 * number + 1]).start()

    def await_all(buffer, number):
        pltpu.make_async_copy(buffer, buffer, sems.at[2 * number + 1]).wait()

    def tell_ids(step, carry):
        send(ids_own, ids_all.at[chip, :, span], 4, lax.rem(ctx + step, ctx_count), member)
        return carry

    lax.fori_loop(1, ctx_count, tell_ids, 0)

    lane = lax.broadcasted_iota(jnp.int32, (blocks, 128), 1)
    loads[4].wait()
    loads[5].wait()
    all_blocks = bss_ref.shape[1]
    scale_row = lax.broadcasted_iota(jnp.int32, (blocks, all_blocks), 0) + member * blocks
    scale_lane = lax.broadcasted_iota(jnp.int32, (blocks, all_blocks), 1)
    second = jnp.sum(
        jnp.where(scale_row == scale_lane, bss_ref[...], 0.0), axis=1, keepdims=True
    )
    for tile in range(3):
        source = [
            (cs_ref[:, tile * 1024 + m * 128 : tile * 1024 + (m + 1) * 128].astype(F32) + 1.0)
            / 256.0
            * second
            for m in range(8)
        ]
        for n in range(8):
            index = 8 * (lane % 16) + n
            picked = take_lanes(source[0], index)
            for m in range(1, 8):
                picked = jnp.where(lane // 16 == m, take_lanes(source[m], index), picked)
            scl[tile * 8 + n] = picked

    at = lax.broadcasted_iota(jnp.int32, (64, tokens), 0)
    feature = (8 * (at % 8) + at // 8).astype(F32)
    position = (lax.broadcasted_iota(jnp.int32, (64, tokens), 1) + chip * tokens).astype(F32)
    angle = position * jnp.exp(feature * (-2.0 * math.log(ROPE_BASE) / HEAD_SIZE))
    cos_ref[...] = jnp.cos(angle)
    sin_ref[...] = jnp.sin(angle)

    pr = lax.broadcasted_iota(jnp.int32, (128, 128), 0)
    pd = lax.broadcasted_iota(jnp.int32, (128, 128), 1)
    perm = (pd == 8 * (pr % 16) + pr // 16).astype(F32).astype(BF16)
    eye_wide = eye(256)

    chunk = 512
    per_chunk = chunk // block_rows
    short_lane = lax.broadcasted_iota(jnp.int32, (block_rows, 128), 1)
    half_lane = lax.broadcasted_iota(jnp.int32, (half_blocks, 128), 1)
    long_lane = lax.broadcasted_iota(jnp.int32, (tokens, 128), 1)
    levels = [jnp.full((block_rows, 128), level, BF16) for level in NF4_LEVELS]
    table = jnp.zeros((block_rows, 128), F32)
    for code, level in enumerate(NF4_LEVELS):
        table = jnp.where(short_lane % 16 == code, F32(level), table)

    def phase(paired, tile, half):
        if paired:
            shift = 16 + 96 * core

            def chosen(lanes):
                return lax.rem(lanes // 16, 2) == core

            def words_at(at):
                return jnp.where(
                    short_lane < 64,
                    codes_ref[pl.ds(at, block_rows), 128:256],
                    codes_ref[pl.ds(at, block_rows), 256:384],
                )
        else:
            shift = 64
            tile_at = pl.multiple_of(tile * 128, 128)

            def chosen(lanes):
                return lanes // 64 == half

            def words_at(at):
                return codes_ref[pl.ds(at, block_rows), pl.ds(tile_at, 128)]

        for n in range(8):
            if paired:
                scale = jnp.where(lane < 64, scl[8 + n], scl[16 + n])
            else:
                scale = scl[tile * 8 + n]
            vscl[n] = jnp.where(
                chosen(half_lane), scale[:half_blocks], pltpu.roll(scale[half_blocks:], shift, 1)
            )
        acc[...] = jnp.zeros_like(acc)
        first = chosen(short_lane)

        def step(k, carry):
            at = pl.multiple_of(member * depth + k * chunk, 128)
            lower = xn[:, pl.ds(at, chunk)]
            upper = xn[:, pl.ds(pl.multiple_of(at + half_depth, 128), chunk)]
            low_words, high_words, full_words = [], [], []
            for b in range(per_chunk):
                row = pl.multiple_of(k * chunk + b * block_rows, block_rows)
                words = jnp.where(
                    first,
                    words_at(row),
                    pltpu.roll(words_at(pl.multiple_of(row + half_depth, block_rows)), shift, 1),
                )
                full_words.append(words)
                low_words.append(words.astype(I16))
                high_words.append(jnp.right_shift(words, 16).astype(I16))
            for pair in range(4):
                planes = []
                for n in (2 * pair, 2 * pair + 1):
                    pieces = []
                    for b in range(per_chunk):
                        scale = vscl[n, pl.ds(k * per_chunk + b, 1), :]
                        if n % 8 in GATHERED:
                            code = jnp.bitwise_and(jnp.right_shift(full_words[b], 4 * n), 15)
                            pieces.append((pick_lanes(table, code) * scale).astype(BF16))
                            continue
                        words = low_words[b] if n < 4 else high_words[b]
                        values = levels
                        for bit in range(4):
                            place = 4 * (n % 4) + bit
                            mark = 1 << place if place < 15 else -(1 << 15)
                            mask = (words & jnp.int16(mark)) != 0
                            values = [
                                jnp.where(mask, values[v + 1], values[v])
                                for v in range(0, len(values), 2)
                            ]
                        pieces.append(values[0] * scale.astype(BF16))
                    planes.append(jnp.concatenate(pieces, axis=0))
                weight = jnp.concatenate(planes, axis=1)
                columns = slice(pair * 256, (pair + 1) * 256)
                acc[0, :, columns] += dot(lower, weight)
                acc[1, :, columns] += dot(upper, weight)
            return carry

        lax.fori_loop(0, half_depth // chunk, step, 0)
        keep = chosen(long_lane)
        for n in range(8):
            columns = slice(n * 128, (n + 1) * 128)
            acct[n] = jnp.where(keep, acc[0, :, columns], acc[1, :, columns]).T

    loads[6].wait()
    copy_x.wait()

    def kv_field(group, part):
        at = pl.multiple_of(64 * group, 64) + 32 * part
        return acct[:, pl.ds(pl.multiple_of(at, 32), 16), :] + acct[
            :, pl.ds(pl.multiple_of(at + 16, 16), 16), :
        ]

    phase(True, 0, 0)
    copy_kv = [None, None]
    for part in (1, 0):
        send_kv[part] = kv_field(partner, part).astype(BF16)
        copy_kv[part] = pair_copy(send_kv.at[part], recv_kv.at[part], 3 + 6 * part, beside)
    for part in range(2):
        own_kv[part] = kv_field(member, part)

    place = 3 * partner + core
    phase(False, place // 2, lax.rem(place, 2))
    send_q[...] = (acct[:, :64, :] + acct[:, 64:, :]).astype(BF16)
    copy_q = pair_copy(send_q, recv_q, 4, beside)

    loads[7].wait()
    loads[8].wait()
    copy_x_rest.wait()
    lr_t = nt(qdown_ref[...], xn[...]).astype(BF16)
    copy_do.wait()
    hold(ids_own, ids_all.at[chip, :, span], 4)
    await_all(ids_all, 4)
    my_ids = ids_all[chip]
    heads = own_q.shape[1] // 16
    local = pl.multiple_of(core * heads * 128, 128)
    marks = lax.broadcasted_iota(jnp.int32, (128, tokens), 0).astype(F32)
    tags = (marks == jnp.broadcast_to(my_ids[:1].astype(F32), (128, tokens))).astype(F32)
    tags = tags.astype(BF16)
    for head in range(heads):
        columns = slice(head * tokens, (head + 1) * tokens)
        queries[128:, columns] = tags
        cotans[:, columns] = nt(perm, do_all[:, head * 128 : (head + 1) * 128]).astype(BF16)

    cosine = cos_ref[...].reshape(8, 8, tokens)
    sine = sin_ref[...].reshape(8, 8, tokens)

    def rotate(field):
        a, b = field[:, :8, :], field[:, 8:, :]
        return jnp.concatenate([a * cosine - b * sine, b * cosine + a * sine], axis=1)

    has_next = outer + 1 < chips // 2

    def send_block(block, part, to_chip):
        half = kv_all.at[block, part]
        pltpu.make_async_remote_copy(
            src_ref=half, dst_ref=half,
            send_sem=block_send.at[0], recv_sem=block_recv.at[2 * block + part],
            device_id=(2 * to_chip + core, member), device_id_type=MESH,
        ).start()

    def await_block(block, part):
        half = kv_all.at[block, part]
        pltpu.make_async_copy(half, half, block_recv.at[2 * block + part]).wait()

    def relay(ahead):
        block = 2 * (outer - 1 - ahead) + inner
        for part in range(2):
            await_block(block, part)

            @pl.when(has_next)
            def _():
                send_block(block, part, chip + 2)

            send_block(block, part, 2 * outer + 1 - inner)

    eye_half = eye(128)
    for part in (1, 0):
        copy_kv[part].wait()
        field = own_kv[part] + recv_kv[part].astype(F32)
        if part == 0:
            field = rotate(field)
        field = field.reshape(128, tokens).astype(BF16)
        kv_all[chip, 1 - part] = tn(field, eye_half).astype(BF16)

        @pl.when(has_next)
        def _():
            send_block(chip, 1 - part, chip + 2)

        @pl.when(inner == 0)
        def _():
            send_block(chip, 1 - part, chip + 1)

    place = 3 * member + core
    phase(False, place // 2, lax.rem(place, 2))
    own_q[...] = acct[:, :64, :] + acct[:, 64:, :]

    @pl.when(outer > 0)
    def _():
        relay(0)

    copy_q.wait()
    for head in range(heads):
        columns = slice(head * tokens, (head + 1) * tokens)
        up_cols = qup_ref[:, pl.ds(pl.multiple_of(local + head * 128, 128), 128)]
        adapter = dot(nt(perm, up_cols).astype(BF16), lr_t).reshape(8, 16, tokens)
        query = own_q[:, 16 * head : 16 * head + 16, :]
        query = query + recv_q[:, 16 * head : 16 * head + 16, :].astype(F32)
        query = query + ADAPTER_SCALE * adapter
        queries[:128, columns] = rotate(query).reshape(128, tokens).astype(BF16)

    soft_scale = 1.0 / math.sqrt(HEAD_SIZE)
    log_scale = soft_scale / math.log(2.0)
    tag_row = lax.broadcasted_iota(jnp.int32, (16, tokens), 0).astype(F32)
    spread_row = lax.broadcasted_iota(jnp.int32, (16, 128), 0)
    spread_lane = lax.broadcasted_iota(jnp.int32, (16, 128), 1)
    spread_tags = (spread_row == spread_lane).astype(F32).astype(BF16)
    vk[256:, :] = jnp.ones((16, tokens), BF16)

    def attend(block, diagonal):
        both = jnp.concatenate([kv_all[block, 0], kv_all[block, 1]], axis=1)
        block_ids = ids_all[block].astype(F32)
        barred = jnp.where(block_ids == tag_row, 0.0, -1e30).astype(BF16)
        barred = tn(barred, spread_tags).astype(BF16)
        lhs = jnp.concatenate([both[:, 128:], barred], axis=1)
        vk[:256, :] = nt(eye_wide, both).astype(BF16)
        tops, decays = [], []
        for head in range(heads):
            columns = slice(head * tokens, (head + 1) * tokens)
            scores = dot(lhs, queries[:, columns]) * log_scale
            if diagonal:
                ki = lax.broadcasted_iota(jnp.int32, (tokens, tokens), 0)
                qi = lax.broadcasted_iota(jnp.int32, (tokens, tokens), 1)
                scores = jnp.where(ki <= qi, scores, -1e30)
            score_buf[head] = scores
            tops.append(jnp.max(scores, axis=0, keepdims=True))
            dots_buf[head] = dot(both[:, :128], cotans[:, columns])
        for head in range(heads):
            row = slice(8 * head, 8 * head + 1)
            top = tops[head]
            if not diagonal:
                before = row_max[row, :]
                top = jnp.maximum(top, before)
                decays.append(jnp.exp2(before - top))
            row_max[row, :] = top
            expo = jnp.exp2(score_buf[head] - top)
            prob_buf[head] = expo.astype(BF16)
            weight_buf[head] = (expo * dots_buf[head]).astype(BF16)
        for head in range(heads):
            new_out = dot(vk[...], prob_buf[head])
            new_grad = dot(vk[128:, :], weight_buf[head])
            if diagonal:
                out_acc[head] = new_out
                grad_acc[head] = new_grad
            else:
                decay = decays[head]
                out_acc[head] = decay * out_acc[head] + new_out
                grad_acc[head] = decay * grad_acc[head] + new_grad

    attend(chip, True)

    def visit(step, carry):
        place = step - inner
        odd = lax.rem(place + 2, 2) == 1
        ahead = (place + 1) // 2

        @pl.when(odd & (ahead > 0) & (ahead < outer))
        def _():
            relay(ahead)

        crossed = 2 * (outer - 1 - (place - 1) // 2) + 1 - inner
        crossed = jnp.where(place < 0, chip - 1, crossed)
        column = 2 * (outer - 1 - place // 2) + inner
        block = jnp.where(odd, crossed, column)

        @pl.when(odd)
        def _():
            await_block(block, 0)
            await_block(block, 1)

        attend(block, False)
        return carry

    lax.fori_loop(0, chip, visit, 0)

    middle = jnp.zeros((16, tokens), F32)
    for head in range(heads):
        inverse = 1.0 / out_acc[head, 256:257, :]
        mean_dot = grad_acc[head, 128:129, :] * inverse
        grad = grad_acc[head, :128, :] - mean_dot * out_acc[head, 128:256, :]
        grad = (soft_scale * inverse * grad).reshape(8, 16, tokens)
        a, b = grad[:, :8, :], grad[:, 8:, :]
        turned = jnp.concatenate([a * cosine + b * sine, b * cosine - a * sine], axis=1)
        lin_t = turned.reshape(128, tokens).astype(BF16)
        lin[head] = lin_t
        up_cols = qup_ref[:, pl.ds(pl.multiple_of(local + head * 128, 128), 128)]
        middle = middle + dot(nt(up_cols, perm).astype(BF16), lin_t)
    mid_own[...] = middle
    quarter = 2 * core + member
    mid_copies = [
        pair_copy(mid_own, mid_in.at[number], 6 + number, device)
        for number, device in enumerate(((ctx, partner), (sibling, partner), (sibling, member)))
    ]

    up_pieces = up_part.shape[0]
    up_stride = chips // up_pieces
    up_mine = chip // up_stride
    owner = lax.rem(chip, up_stride) == 0
    up_slot = core * up_pieces + up_mine
    ga_slot = quarter * up_pieces + up_mine
    low = chip < chips // 2

    def far_first(step, count):
        return jnp.where(low, count - 1 - step, step)

    back = 16 * (pd % 8) + pd // 8
    for head in range(heads):
        up = take_lanes(ADAPTER_SCALE * nt(lr_t, lin[head]), back[:16])
        up_part[2 * head] = up[:8]
        up_part[2 * head + 1] = up[8:]

    def scatter(part, into, number):
        def one(step, carry):
            j = far_first(step, up_pieces)
            to = j * up_stride

            @pl.when(to != chip)
            def _():
                send(part.at[j], into.at[chip], number, 2 * to + core, member)

            return carry

        lax.fori_loop(0, up_pieces, one, 0)

        @pl.when(owner)
        def _():
            hold(part.at[up_mine], into.at[chip], number)

    scatter(up_part, up_in, 0)

    for head in range(heads):
        inverse = 1.0 / out_acc[head, 256:257, :]
        out = (out_acc[head, :128, :] * inverse).astype(BF16)
        out_stage[:, head * 128 : (head + 1) * 128] = tn(out, perm).astype(BF16)

    for copy in mid_copies:
        copy.wait()
    middle = mid_own[...] + mid_in[0] + mid_in[1] + mid_in[2]
    middle = (ADAPTER_SCALE * middle).astype(BF16)
    share = up_pieces * 128
    ga = dot(middle, xn[:, pl.ds(pl.multiple_of(quarter * share, 128), share)])
    for j in range(up_pieces):
        ga_part[j] = ga[:, j * 128 : (j + 1) * 128].astype(BF16)
    scatter(ga_part, ga_in, 1)

    copy_out = pair_copy(out_stage.at[pl.ds(other_at, rows)], out_in, 5, across)
    out_ref[:, pl.ds(mine_columns, half_columns)] = out_stage[pl.ds(mine_at, rows), :]

    @pl.when(owner)
    def _():
        await_all(up_in, 0)
        up_sum[...] = jnp.sum(up_in[...], axis=0)

        def spread_up(step, carry):
            to = far_first(step, ctx_count)

            @pl.when(to != ctx)
            def _():
                send(up_sum, up_all.at[up_slot], 2, to, member)

            return carry

        lax.fori_loop(0, ctx_count, spread_up, 0)
        hold(up_sum, up_all.at[up_slot], 2)

        await_all(ga_in, 1)
        ga_sum[...] = jnp.sum(ga_in[...].astype(F32), axis=0).astype(BF16)

        def spread_ga(step, carry):
            place = far_first(step, total)
            to, to_fsdp = place // fsdp_count, lax.rem(place, fsdp_count)

            @pl.when(place != me)
            def _():
                send(ga_sum, ga_all.at[ga_slot], 3, to, to_fsdp)

            return carry

        lax.fori_loop(0, total, spread_ga, 0)
        hold(ga_sum, ga_all.at[ga_slot], 3)

    copy_out.wait()
    out_ref[:, pl.ds(other_columns, half_columns)] = out_in[...]

    await_all(up_all, 2)
    for j in range(2 * up_pieces):
        row, col = 8 * (j % 2), 128 * (j // 2)
        up_out[row : row + 8, col : col + 128] = up_all[j]
    await_all(ga_all, 3)
    for j in range(4 * up_pieces):
        ga_out[:, j * 128 : (j + 1) * 128] = ga_all[j].astype(F32)

    def drain(buffer, semaphore, sent):
        def one(step, carry):
            pltpu.make_async_copy(buffer, buffer, semaphore).wait()
            return carry

        lax.fori_loop(0, sent, one, 0)

    onward = has_next.astype(jnp.int32)
    passed = 2 * (onward + 1 - inner + outer * (onward + 1))
    drain(kv_all.at[chip, 0], block_send.at[0], passed)
    scattered = up_pieces - owner.astype(jnp.int32)
    drain(up_part.at[0], sems.at[0], scattered)
    drain(ga_part.at[0], sems.at[2], scattered)
    drain(up_sum, sems.at[4], jnp.where(owner, ctx_count - 1, 0))
    drain(ga_sum, sems.at[6], jnp.where(owner, total - 1, 0))
    drain(ids_own, sems.at[8], ctx_count - 1)


def store_kernel(attn_ref, ga_ref, up_ref, attn_out, ga_out, up_out, sems):
    copies = [
        pltpu.make_async_copy(src, dst, sems.at[number])
        for number, (src, dst) in enumerate(
            ((attn_ref, attn_out), (ga_ref, ga_out), (up_ref, up_out))
        )
    ]
    for copy in copies:
        copy.start()
    for copy in copies:
        copy.wait()


def on_device(
    counts, layer_input, gain, codes, column_scale_quantized, block_second_scale,
    query_down_map, query_up_map, token_document, output_cotangent,
):
    ctx_count, fsdp_count = counts
    total = ctx_count * fsdp_count
    chips = ctx_count // 2
    rows, width = layer_input.shape
    tokens = 2 * rows
    vm = pl.BlockSpec(memory_space=pltpu.VMEM)
    hbm = pl.BlockSpec(memory_space=pltpu.HBM)
    blocks = column_scale_quantized.shape[0]
    rank, local_columns = query_up_map.shape
    heads = local_columns // HEAD_SIZE // 2
    up_pieces = 2 * heads
    vmem, dma = pltpu.VMEM, pltpu.SemaphoreType.DMA
    attn, ga, up = pl.pallas_call(
        functools.partial(step_kernel, counts),
        out_shape=(
            vmem(output_cotangent.shape, BF16),
            vmem((rank, width), F32),
            vmem(query_up_map.shape, F32),
        ),
        in_specs=[hbm] * 9,
        out_specs=(vm,) * 3,
        scratch_shapes=[
            vmem(layer_input.shape, BF16),
            vmem((1, width), F32),
            vmem(codes.shape, jnp.int32),
            vmem(column_scale_quantized.shape, jnp.int32),
            vmem((1, block_second_scale.shape[0]), F32),
            vmem((rank, width), BF16),
            vmem(query_up_map.shape, BF16),
            vmem((1, rows), jnp.int32),
            vmem(output_cotangent.shape, BF16),
            vmem((24, blocks, 128), F32),
            vmem((8, blocks // 2, 128), F32),
            vmem((2, tokens, 1024), F32),
            vmem((8, 128, tokens), F32),
            vmem((tokens, width), BF16),
            vmem((HEAD_SIZE // 2, tokens), F32),
            vmem((HEAD_SIZE // 2, tokens), F32),
            vmem((2, 8, 16, tokens), F32),
            vmem((2, 8, 16, tokens), BF16),
            vmem((2, 8, 16, tokens), BF16),
            vmem((8, 16 * heads, tokens), F32),
            vmem((8, 16 * heads, tokens), BF16),
            vmem((8, 16 * heads, tokens), BF16),
            vmem((tokens, heads * 128), BF16),
            vmem((16, rows), BF16),
            vmem((chips, 16, tokens), BF16),
            vmem((chips, 2, tokens, 128), BF16),
            vmem((256, heads * tokens), BF16),
            vmem((128, heads * tokens), BF16),
            vmem((256 + 16, tokens), BF16),
            vmem((8 * heads, tokens), F32),
            vmem((heads, 256 + 16, tokens), F32),
            vmem((heads, 128 + 16, tokens), F32),
            vmem((heads, 128, tokens), BF16),
            vmem((heads, tokens, tokens), F32),
            vmem((heads, tokens, tokens), F32),
            vmem((heads, tokens, tokens), BF16),
            vmem((heads, tokens, tokens), BF16),
            vmem((tokens, heads * 128), BF16),
            vmem((rows, heads * 128), BF16),
            vmem((rank, tokens), F32),
            vmem((3, rank, tokens), F32),
            vmem((up_pieces, rank, 128), BF16),
            vmem((chips, rank, 128), BF16),
            vmem((rank, 128), BF16),
            vmem((4 * up_pieces, rank, 128), BF16),
            vmem((up_pieces, 8, 128), F32),
            vmem((chips, 8, 128), F32),
            vmem((8, 128), F32),
            vmem((2 * up_pieces, 8, 128), F32),
            dma((9,)),
            dma((10,)),
            dma((10,)),
            dma((1,)),
            dma((2 * chips,)),
            dma((10,)),
        ],
        compiler_params=pltpu.CompilerParams(
            collective_id=0, has_side_effects=True, vmem_limit_bytes=56 * 1024 * 1024
        ),
        name="step",
    )(
        layer_input, gain[None, :], codes, column_scale_quantized, block_second_scale[None, :],
        query_down_map.T, query_up_map, token_document[None, :], output_cotangent,
    )
    attn, ga, up = pl.pallas_call(
        store_kernel,
        out_shape=tuple(jax.ShapeDtypeStruct(a.shape, a.dtype) for a in (attn, ga, up)),
        in_specs=[vm] * 3,
        out_specs=(hbm,) * 3,
        scratch_shapes=[dma((3,))],
        compiler_params=pltpu.CompilerParams(vmem_limit_bytes=4 * 1024 * 1024),
        name="store",
    )(attn, ga, up)
    return attn, ga.T, up


def solution(mesh):
    return jax.shard_map(
        functools.partial(on_device, (mesh.shape["ctx"], mesh.shape["fsdp"])),
        mesh=mesh,
        in_specs=(
            P("ctx", None),
            P(),
            P("fsdp", None),
            P("fsdp", None),
            P(),
            P(),
            P(None, "fsdp"),
            P("ctx"),
            P("ctx", "fsdp"),
        ),
        out_specs=(P("ctx", "fsdp"), P(), P(None, "fsdp")),
        check_vma=False,
    )
```

```python
import math
import functools

import jax
import jax.numpy as jnp
from jax import lax
from jax.experimental import pallas as pl
from jax.experimental.pallas import tpu as pltpu
from jax.sharding import PartitionSpec as P

HEAD_SIZE = 128
ADAPTER_SCALE = 2.0
ROPE_BASE = 500000.0
MESH = pl.DeviceIdType.MESH
F32 = jnp.float32
BF16 = jnp.bfloat16
I16 = jnp.int16

NF4_LEVELS = [
    -1.0,
    -0.6961928009986877,
    -0.5250730514526367,
    -0.39491748809814453,
    -0.28444138169288635,
    -0.18477343022823334,
    -0.09105003625154495,
    0.0,
    0.07958029955625534,
    0.16093020141124725,
    0.24611230194568634,
    0.33791524171829224,
    0.44070982933044434,
    0.5626170039176941,
    0.7229568362236023,
    1.0,
]


def take_lanes(values, index):
    return jnp.take_along_axis(values, index, axis=1, mode="promise_in_bounds")


GATHERED = (1, 3, 5, 7)
LANE_PICK = lax.GatherDimensionNumbers(
    offset_dims=(), collapsed_slice_dims=(1,), start_index_map=(1,),
    operand_batching_dims=(0,), start_indices_batching_dims=(0,),
)


def pick_lanes(values, index):
    return lax.gather(
        values, index[..., None], LANE_PICK, (1, 1),
        mode=lax.GatherScatterMode.PROMISE_IN_BOUNDS,
    )


def dot(a, b):
    return jnp.dot(a, b, preferred_element_type=F32)


def nt(a, b):
    return lax.dot_general(a, b, (((1,), (1,)), ((), ())), preferred_element_type=F32)


def tn(a, b):
    return lax.dot_general(a, b, (((0,), (0,)), ((), ())), preferred_element_type=F32)


def eye(size):
    row = lax.broadcasted_iota(jnp.int32, (size, size), 0)
    col = lax.broadcasted_iota(jnp.int32, (size, size), 1)
    return (row == col).astype(F32).astype(BF16)


def step_kernel(
    counts,
    x_hbm, gain_hbm, codes_hbm, cs_hbm, bss_hbm, qdown_hbm, qup_hbm, ids_hbm, do_hbm,
    out_ref, ga_out, up_out,
    x_ref, gain_ref, codes_ref, cs_ref, bss_ref, qdown_ref, qup_ref, ids_ref, do_ref, scl, vscl, weights, acc, acct, xn, cos_ref, sin_ref, own_kv, send_kv, recv_kv, own_q, send_q, recv_q,
    do_all, ids_own, ids_all, kv_all, queries, cotans, vk, row_max, out_acc, grad_acc, lin,
    score_buf, dots_buf, prob_buf, weight_buf, out_stage, out_in, mid_own, mid_in,
    ga_part, ga_in, ga_sum, ga_all, up_part, up_in, up_sum, up_all,
    load, pair_send, pair_recv, block_send, block_recv, sems,
):
    early = x_hbm.shape[0] // 2
    loads = [
        pltpu.make_async_copy(src, dst, load.at[number])
        for number, (src, dst) in enumerate(
            (
                (x_hbm.at[:early], x_ref.at[:early]), (gain_hbm, gain_ref), (ids_hbm, ids_ref),
                (do_hbm, do_ref),
                (bss_hbm, bss_ref), (cs_hbm, cs_ref), (codes_hbm, codes_ref),
                (qdown_hbm, qdown_ref), (qup_hbm, qup_ref), (x_hbm.at[early:], x_ref.at[early:]),
            )
        )
    ]
    for number in (0, 1, 9, 2, 3, 4, 5, 6, 7, 8):
        loads[number].start()
    ctx_count, fsdp_count = counts
    total = ctx_count * fsdp_count
    ctx, member = lax.axis_index("ctx"), lax.axis_index("fsdp")
    me = ctx * fsdp_count + member
    partner = 1 - member
    chip, core = ctx // 2, lax.rem(ctx, 2)
    outer, inner = chip // 2, lax.rem(chip, 2)
    sibling = ctx + 1 - 2 * core
    chips = ctx_count // 2
    rows, width = x_ref.shape
    tokens = 2 * rows
    depth = codes_ref.shape[0]
    half_depth = depth // 2
    blocks = cs_ref.shape[0]
    block_rows = depth // blocks
    half_blocks = blocks // 2

    barrier = pltpu.get_barrier_semaphore()

    low = chip < chips // 2

    def far_first(step, count):
        return jnp.where(low, count - 1 - step, step)

    def greet(step, carry):
        other = far_first(step, total)

        @pl.when(other != me)
        def _():
            pl.semaphore_signal(
                barrier, inc=1, device_id=(other // fsdp_count, lax.rem(other, fsdp_count)),
                device_id_type=MESH,
            )

        return carry

    lax.fori_loop(0, total, greet, 0)

    mine_at = pl.multiple_of(core * rows, rows)
    other_at = pl.multiple_of((1 - core) * rows, rows)
    loads[0].wait()
    loads[1].wait()
    for r in range(0, rows, 16):
        if r == early:
            loads[9].wait()
        wide = x_ref[r : r + 16, :].astype(F32)
        inverse = lax.rsqrt(jnp.mean(wide * wide, axis=-1, keepdims=True) + 1e-05)
        xn[pl.ds(pl.multiple_of(mine_at + r, 16), 16), :] = (
            wide * inverse * gain_ref[...]
        ).astype(BF16)
    loads[2].wait()
    ids_own[...] = jnp.broadcast_to(
        ids_ref[...].astype(F32), (16, rows)
    ).astype(BF16)
    half_columns = do_ref.shape[1] // 2
    mine_columns = pl.multiple_of(core * half_columns, 128)
    other_columns = pl.multiple_of((1 - core) * half_columns, 128)
    loads[3].wait()
    do_all[pl.ds(mine_at, rows), :] = do_ref[:, pl.ds(mine_columns, half_columns)]

    lane = lax.broadcasted_iota(jnp.int32, (blocks, 128), 1)
    loads[4].wait()
    loads[5].wait()
    all_blocks = bss_ref.shape[1]
    scale_row = lax.broadcasted_iota(jnp.int32, (blocks, all_blocks), 0) + member * blocks
    scale_lane = lax.broadcasted_iota(jnp.int32, (blocks, all_blocks), 1)
    second = jnp.sum(
        jnp.where(scale_row == scale_lane, bss_ref[...], 0.0), axis=1, keepdims=True
    )
    for tile in range(3):
        source = [
            (cs_ref[:, tile * 1024 + m * 128 : tile * 1024 + (m + 1) * 128].astype(F32) + 1.0)
            / 256.0
            * second
            for m in range(8)
        ]
        for n in range(8):
            index = 8 * (lane % 16) + n
            picked = take_lanes(source[0], index)
            for m in range(1, 8):
                picked = jnp.where(lane // 16 == m, take_lanes(source[m], index), picked)
            scl[tile * 8 + n] = picked

    pl.semaphore_wait(barrier, total - 1)

    def pair_copy(src, dst, number, device):
        copy = pltpu.make_async_remote_copy(
            src_ref=src, dst_ref=dst, send_sem=pair_send.at[number],
            recv_sem=pair_recv.at[number], device_id=device, device_id_type=MESH,
        )
        copy.start()
        return copy

    across = (sibling, member)
    beside = (ctx, partner)
    span = pl.ds(mine_at, rows)
    near = xn.at[span, pl.ds(pl.multiple_of(member * depth, 128), depth)]
    far = xn.at[span, pl.ds(pl.multiple_of(partner * depth, 128), depth)]
    copy_x = pair_copy(near, near, 0, across)
    copy_x_rest = pair_copy(far, far, 1, across)
    copy_do = pair_copy(
        do_ref.at[:, pl.ds(other_columns, half_columns)], do_all.at[span], 2, across
    )

    def send(src, dst, number, ctx_to, fsdp_to):
        pltpu.make_async_remote_copy(
            src_ref=src, dst_ref=dst, send_sem=sems.at[2 * number],
            recv_sem=sems.at[2 * number + 1], device_id=(ctx_to, fsdp_to),
            device_id_type=MESH,
        ).start()

    def hold(src, dst, number):
        pltpu.make_async_copy(src, dst, sems.at[2 * number + 1]).start()

    def await_all(buffer, number):
        pltpu.make_async_copy(buffer, buffer, sems.at[2 * number + 1]).wait()

    def tell_ids(step, carry):
        send(ids_own, ids_all.at[chip, :, span], 4, lax.rem(ctx + step, ctx_count), member)
        return carry

    lax.fori_loop(1, ctx_count, tell_ids, 0)

    at = lax.broadcasted_iota(jnp.int32, (64, tokens), 0)
    feature = (8 * (at % 8) + at // 8).astype(F32)
    position = (lax.broadcasted_iota(jnp.int32, (64, tokens), 1) + chip * tokens).astype(F32)
    angle = position * jnp.exp(feature * (-2.0 * math.log(ROPE_BASE) / HEAD_SIZE))
    cos_ref[...] = jnp.cos(angle)
    sin_ref[...] = jnp.sin(angle)

    pr = lax.broadcasted_iota(jnp.int32, (128, 128), 0)
    pd = lax.broadcasted_iota(jnp.int32, (128, 128), 1)
    perm = (pd == 8 * (pr % 16) + pr // 16).astype(F32).astype(BF16)
    eye_wide = eye(256)

    chunk = 512
    per_chunk = chunk // block_rows
    short_lane = lax.broadcasted_iota(jnp.int32, (block_rows, 128), 1)
    half_lane = lax.broadcasted_iota(jnp.int32, (half_blocks, 128), 1)
    long_lane = lax.broadcasted_iota(jnp.int32, (tokens, 128), 1)
    levels = [jnp.full((block_rows, 128), level, BF16) for level in NF4_LEVELS]
    table = jnp.zeros((block_rows, 128), F32)
    for code, level in enumerate(NF4_LEVELS):
        table = jnp.where(short_lane % 16 == code, F32(level), table)

    def phase(paired, tile, half, ready=None):
        if paired:
            shift = 16 + 96 * core

            def chosen(lanes):
                return lax.rem(lanes // 16, 2) == core

            def words_at(at):
                return jnp.where(
                    short_lane < 64,
                    codes_ref[pl.ds(at, block_rows), 128:256],
                    codes_ref[pl.ds(at, block_rows), 256:384],
                )
        else:
            shift = 64
            tile_at = pl.multiple_of(tile * 128, 128)

            def chosen(lanes):
                return lanes // 64 == half

            def words_at(at):
                return codes_ref[pl.ds(at, block_rows), pl.ds(tile_at, 128)]

        for n in range(8):
            if paired:
                scale = jnp.where(lane < 64, scl[8 + n], scl[16 + n])
            else:
                scale = scl[tile * 8 + n]
            vscl[n] = jnp.where(
                chosen(half_lane), scale[:half_blocks], pltpu.roll(scale[half_blocks:], shift, 1)
            )
        if ready is None:
            acc[...] = jnp.zeros_like(acc)
        first = chosen(short_lane)

        def step(k, carry):
            if ready is None:
                at = pl.multiple_of(member * depth + k * chunk, 128)
                lower = xn[:, pl.ds(at, chunk)]
                upper = xn[:, pl.ds(pl.multiple_of(at + half_depth, 128), chunk)]
            low_words, high_words, full_words = [], [], []
            for b in range(per_chunk):
                row = pl.multiple_of(k * chunk + b * block_rows, block_rows)
                words = jnp.where(
                    first,
                    words_at(row),
                    pltpu.roll(words_at(pl.multiple_of(row + half_depth, block_rows)), shift, 1),
                )
                full_words.append(words)
                low_words.append(words.astype(I16))
                high_words.append(jnp.right_shift(words, 16).astype(I16))
            for pair in range(4):
                planes = []
                for n in (2 * pair, 2 * pair + 1):
                    pieces = []
                    for b in range(per_chunk):
                        scale = vscl[n, pl.ds(k * per_chunk + b, 1), :]
                        if n % 8 in GATHERED:
                            code = jnp.bitwise_and(jnp.right_shift(full_words[b], 4 * n), 15)
                            pieces.append((pick_lanes(table, code) * scale).astype(BF16))
                            continue
                        words = low_words[b] if n < 4 else high_words[b]
                        values = levels
                        for bit in range(4):
                            place = 4 * (n % 4) + bit
                            mark = 1 << place if place < 15 else -(1 << 15)
                            mask = (words & jnp.int16(mark)) != 0
                            values = [
                                jnp.where(mask, values[v + 1], values[v])
                                for v in range(0, len(values), 2)
                            ]
                        pieces.append(values[0] * scale.astype(BF16))
                    planes.append(jnp.concatenate(pieces, axis=0))
                weight = jnp.concatenate(planes, axis=1)
                columns = slice(pair * 256, (pair + 1) * 256)
                if ready is None:
                    acc[0, :, columns] += dot(lower, weight)
                    acc[1, :, columns] += dot(upper, weight)
                else:
                    weights[pl.ds(pl.multiple_of(k * chunk, chunk), chunk), columns] = weight
            return carry

        lax.fori_loop(0, half_depth // chunk, step, 0)
        if ready is not None:
            ready()
            for side in range(2):
                at = pl.multiple_of(member * depth + side * half_depth, 128)
                for pair in range(4):
                    columns = slice(pair * 256, (pair + 1) * 256)
                    acc[side, :, columns] = dot(xn[:, pl.ds(at, half_depth)], weights[:, columns])
        keep = chosen(long_lane)
        for n in range(8):
            columns = slice(n * 128, (n + 1) * 128)
            acct[n] = jnp.where(keep, acc[0, :, columns], acc[1, :, columns]).T

    loads[6].wait()

    def kv_field(group, part):
        at = pl.multiple_of(64 * group, 64) + 32 * part
        return acct[:, pl.ds(pl.multiple_of(at, 32), 16), :] + acct[
            :, pl.ds(pl.multiple_of(at + 16, 16), 16), :
        ]

    phase(True, 0, 0, copy_x.wait)
    copy_kv = [None, None]
    for part in (1, 0):
        send_kv[part] = kv_field(partner, part).astype(BF16)
        copy_kv[part] = pair_copy(send_kv.at[part], recv_kv.at[part], 3 + 6 * part, beside)
    for part in range(2):
        own_kv[part] = kv_field(member, part)

    place = 3 * partner + core
    phase(False, place // 2, lax.rem(place, 2))
    send_q[...] = (acct[:, :64, :] + acct[:, 64:, :]).astype(BF16)
    copy_q = pair_copy(send_q, recv_q, 4, beside)

    loads[7].wait()
    loads[8].wait()
    copy_x_rest.wait()
    lr_t = nt(qdown_ref[...], xn[...]).astype(BF16)
    copy_do.wait()
    hold(ids_own, ids_all.at[chip, :, span], 4)
    await_all(ids_all, 4)
    my_ids = ids_all[chip]
    heads = own_q.shape[1] // 16
    local = pl.multiple_of(core * heads * 128, 128)
    marks = lax.broadcasted_iota(jnp.int32, (128, tokens), 0).astype(F32)
    tags = (marks == jnp.broadcast_to(my_ids[:1].astype(F32), (128, tokens))).astype(F32)
    tags = tags.astype(BF16)
    for head in range(heads):
        columns = slice(head * tokens, (head + 1) * tokens)
        queries[128:, columns] = tags
        cotans[:, columns] = nt(perm, do_all[:, head * 128 : (head + 1) * 128]).astype(BF16)

    cosine = cos_ref[...].reshape(8, 8, tokens)
    sine = sin_ref[...].reshape(8, 8, tokens)

    def rotate(field):
        a, b = field[:, :8, :], field[:, 8:, :]
        return jnp.concatenate([a * cosine - b * sine, b * cosine + a * sine], axis=1)

    has_next = outer + 1 < chips // 2

    def send_block(block, part, to_chip):
        half = kv_all.at[block, part]
        pltpu.make_async_remote_copy(
            src_ref=half, dst_ref=half,
            send_sem=block_send.at[0], recv_sem=block_recv.at[2 * block + part],
            device_id=(2 * to_chip + core, member), device_id_type=MESH,
        ).start()

    def await_block(block, part):
        half = kv_all.at[block, part]
        pltpu.make_async_copy(half, half, block_recv.at[2 * block + part]).wait()

    def relay(ahead, parts=(0, 1)):
        block = 2 * (outer - 1 - ahead) + inner
        for part in parts:
            await_block(block, part)

            @pl.when(has_next)
            def _():
                send_block(block, part, chip + 2)

            send_block(block, part, 2 * outer + 1 - inner)

    eye_half = eye(128)
    for part in (1, 0):
        copy_kv[part].wait()
        field = own_kv[part] + recv_kv[part].astype(F32)
        if part == 0:
            field = rotate(field)
        field = field.reshape(128, tokens).astype(BF16)
        kv_all[chip, 1 - part] = tn(field, eye_half).astype(BF16)

        @pl.when(has_next)
        def _():
            send_block(chip, 1 - part, chip + 2)

        @pl.when(inner == 0)
        def _():
            send_block(chip, 1 - part, chip + 1)

    place = 3 * member + core
    phase(False, place // 2, lax.rem(place, 2))
    own_q[...] = acct[:, :64, :] + acct[:, 64:, :]

    @pl.when(outer > 0)
    def _():
        relay(0)

    @pl.when(outer > 1)
    def _():
        relay(1, (0,))

    copy_q.wait()
    for head in range(heads):
        columns = slice(head * tokens, (head + 1) * tokens)
        up_cols = qup_ref[:, pl.ds(pl.multiple_of(local + head * 128, 128), 128)]
        adapter = dot(nt(perm, up_cols).astype(BF16), lr_t).reshape(8, 16, tokens)
        query = own_q[:, 16 * head : 16 * head + 16, :]
        query = query + recv_q[:, 16 * head : 16 * head + 16, :].astype(F32)
        query = query + ADAPTER_SCALE * adapter
        queries[:128, columns] = rotate(query).reshape(128, tokens).astype(BF16)

    @pl.when(outer > 1)
    def _():
        relay(1, (1,))

    soft_scale = 1.0 / math.sqrt(HEAD_SIZE)
    log_scale = soft_scale / math.log(2.0)
    tag_row = lax.broadcasted_iota(jnp.int32, (16, tokens), 0).astype(F32)
    spread_row = lax.broadcasted_iota(jnp.int32, (16, 128), 0)
    spread_lane = lax.broadcasted_iota(jnp.int32, (16, 128), 1)
    spread_tags = (spread_row == spread_lane).astype(F32).astype(BF16)
    vk[256:, :] = jnp.ones((16, tokens), BF16)

    def attend(block, diagonal):
        both = jnp.concatenate([kv_all[block, 0], kv_all[block, 1]], axis=1)
        block_ids = ids_all[block].astype(F32)
        barred = jnp.where(block_ids == tag_row, 0.0, -1e30).astype(BF16)
        barred = tn(barred, spread_tags).astype(BF16)
        lhs = jnp.concatenate([both[:, 128:], barred], axis=1)
        vk[:256, :] = nt(eye_wide, both).astype(BF16)
        tops, decays = [], []
        for head in range(heads):
            columns = slice(head * tokens, (head + 1) * tokens)
            scores = dot(lhs, queries[:, columns]) * log_scale
            if diagonal:
                ki = lax.broadcasted_iota(jnp.int32, (tokens, tokens), 0)
                qi = lax.broadcasted_iota(jnp.int32, (tokens, tokens), 1)
                scores = jnp.where(ki <= qi, scores, -1e30)
            score_buf[head] = scores
            tops.append(jnp.max(scores, axis=0, keepdims=True))
            dots_buf[head] = dot(both[:, :128], cotans[:, columns])
        for head in range(heads):
            row = slice(8 * head, 8 * head + 1)
            top = tops[head]
            if not diagonal:
                before = row_max[row, :]
                top = jnp.maximum(top, before)
                decays.append(jnp.exp2(before - top))
            row_max[row, :] = top
            expo = jnp.exp2(score_buf[head] - top)
            prob_buf[head] = expo.astype(BF16)
            weight_buf[head] = (expo * dots_buf[head]).astype(BF16)
        for head in range(heads):
            new_out = dot(vk[...], prob_buf[head])
            new_grad = dot(vk[128:, :], weight_buf[head])
            if diagonal:
                out_acc[head] = new_out
                grad_acc[head] = new_grad
            else:
                decay = decays[head]
                out_acc[head] = decay * out_acc[head] + new_out
                grad_acc[head] = decay * grad_acc[head] + new_grad

    attend(chip, True)

    def visit(step, carry):
        place = step - inner
        odd = lax.rem(place + 2, 2) == 1
        ahead = step // 2 + 1

        @pl.when((lax.rem(step, 2) == 0) & (ahead > 1) & (ahead < outer))
        def _():
            relay(ahead)

        crossed = 2 * (outer - 1 - (place - 1) // 2) + 1 - inner
        crossed = jnp.where(place < 0, chip - 1, crossed)
        column = 2 * (outer - 1 - place // 2) + inner
        block = jnp.where(odd, crossed, column)

        @pl.when(odd)
        def _():
            await_block(block, 0)
            await_block(block, 1)

        attend(block, False)
        return carry

    lax.fori_loop(0, chip, visit, 0)

    middle = jnp.zeros((16, tokens), F32)
    for head in range(heads):
        inverse = 1.0 / out_acc[head, 256:257, :]
        mean_dot = grad_acc[head, 128:129, :] * inverse
        grad = grad_acc[head, :128, :] - mean_dot * out_acc[head, 128:256, :]
        grad = (soft_scale * inverse * grad).reshape(8, 16, tokens)
        a, b = grad[:, :8, :], grad[:, 8:, :]
        turned = jnp.concatenate([a * cosine + b * sine, b * cosine - a * sine], axis=1)
        lin_t = turned.reshape(128, tokens).astype(BF16)
        lin[head] = lin_t
        up_cols = qup_ref[:, pl.ds(pl.multiple_of(local + head * 128, 128), 128)]
        middle = middle + dot(nt(up_cols, perm).astype(BF16), lin_t)
    mid_own[...] = middle
    quarter = 2 * core + member
    mid_copies = [
        pair_copy(mid_own, mid_in.at[number], 6 + number, device)
        for number, device in enumerate(((ctx, partner), (sibling, partner), (sibling, member)))
    ]

    owners, per = up_part.shape[:2]
    stride = chips // 2 // owners
    first_owner = chips // 4
    turn = chip - first_owner
    mine = turn // stride
    owner = (turn >= 0) & (turn < owners * stride) & (lax.rem(turn + chips, stride) == 0)
    up_slot = core * owners + mine
    ga_slot = quarter * owners + mine
    back = 16 * (pd % 8) + pd // 8
    for head in range(heads):
        up = take_lanes(ADAPTER_SCALE * nt(lr_t, lin[head]), back[:16])
        for part in range(2):
            piece = 2 * head + part
            up_part[piece // per, piece % per] = up[8 * part : 8 * part + 8]

    def scatter(part, into, number):
        def one(step, carry):
            j = far_first(step, owners)
            to = first_owner + j * stride

            @pl.when(to != chip)
            def _():
                send(part.at[j], into.at[chip], number, 2 * to + core, member)

            return carry

        lax.fori_loop(0, owners, one, 0)

        @pl.when(owner)
        def _():
            hold(part.at[mine], into.at[chip], number)

    scatter(up_part, up_in, 0)

    for head in range(heads):
        inverse = 1.0 / out_acc[head, 256:257, :]
        out = (out_acc[head, :128, :] * inverse).astype(BF16)
        out_stage[:, head * 128 : (head + 1) * 128] = tn(out, perm).astype(BF16)

    for copy in mid_copies:
        copy.wait()
    middle = mid_own[...] + mid_in[0] + mid_in[1] + mid_in[2]
    middle = (ADAPTER_SCALE * middle).astype(BF16)
    share = owners * per * 128
    ga = dot(middle, xn[:, pl.ds(pl.multiple_of(quarter * share, 128), share)])
    for j in range(owners * per):
        ga_part[j // per, j % per] = ga[:, j * 128 : (j + 1) * 128].astype(BF16)
    scatter(ga_part, ga_in, 1)

    copy_out = pair_copy(out_stage.at[pl.ds(other_at, rows)], out_in, 5, across)
    out_ref[:, pl.ds(mine_columns, half_columns)] = out_stage[pl.ds(mine_at, rows), :]

    @pl.when(owner)
    def _():
        await_all(up_in, 0)
        up_sum[...] = jnp.sum(up_in[...], axis=0)

        def spread_up(step, carry):
            to = far_first(step, ctx_count)

            @pl.when(to != ctx)
            def _():
                send(up_sum, up_all.at[up_slot], 2, to, member)

            return carry

        lax.fori_loop(0, ctx_count, spread_up, 0)
        hold(up_sum, up_all.at[up_slot], 2)

        await_all(ga_in, 1)
        ga_sum[...] = jnp.sum(ga_in[...].astype(F32), axis=0).astype(BF16)

        def spread_ga(step, carry):
            place = far_first(step, total)
            to, to_fsdp = place // fsdp_count, lax.rem(place, fsdp_count)

            @pl.when(place != me)
            def _():
                send(ga_sum, ga_all.at[ga_slot], 3, to, to_fsdp)

            return carry

        lax.fori_loop(0, total, spread_ga, 0)
        hold(ga_sum, ga_all.at[ga_slot], 3)

    copy_out.wait()
    out_ref[:, pl.ds(other_columns, half_columns)] = out_in[...]

    await_all(up_all, 2)
    for j in range(2 * owners * per):
        row, col = 8 * (j % 2), 128 * (j // 2)
        up_out[row : row + 8, col : col + 128] = up_all[j // per, j % per]
    await_all(ga_all, 3)
    for j in range(4 * owners * per):
        ga_out[:, j * 128 : (j + 1) * 128] = ga_all[j // per, j % per].astype(F32)

    def drain(buffer, semaphore, sent):
        def one(step, carry):
            pltpu.make_async_copy(buffer, buffer, semaphore).wait()
            return carry

        lax.fori_loop(0, sent, one, 0)

    onward = has_next.astype(jnp.int32)
    passed = 2 * (onward + 1 - inner + outer * (onward + 1))
    drain(kv_all.at[chip, 0], block_send.at[0], passed)
    scattered = owners - owner.astype(jnp.int32)
    drain(up_part.at[0], sems.at[0], scattered)
    drain(ga_part.at[0], sems.at[2], scattered)
    drain(up_sum, sems.at[4], jnp.where(owner, ctx_count - 1, 0))
    drain(ga_sum, sems.at[6], jnp.where(owner, total - 1, 0))
    drain(ids_own, sems.at[8], ctx_count - 1)


def store_kernel(attn_ref, ga_ref, up_ref, attn_out, ga_out, up_out, sems):
    copies = [
        pltpu.make_async_copy(src, dst, sems.at[number])
        for number, (src, dst) in enumerate(
            ((attn_ref, attn_out), (ga_ref, ga_out), (up_ref, up_out))
        )
    ]
    for copy in copies:
        copy.start()
    for copy in copies:
        copy.wait()


def on_device(
    counts, layer_input, gain, codes, column_scale_quantized, block_second_scale,
    query_down_map, query_up_map, token_document, output_cotangent,
):
    ctx_count, fsdp_count = counts
    total = ctx_count * fsdp_count
    chips = ctx_count // 2
    rows, width = layer_input.shape
    tokens = 2 * rows
    vm = pl.BlockSpec(memory_space=pltpu.VMEM)
    hbm = pl.BlockSpec(memory_space=pltpu.HBM)
    blocks = column_scale_quantized.shape[0]
    rank, local_columns = query_up_map.shape
    heads = local_columns // HEAD_SIZE // 2
    owners = math.gcd(2 * heads, chips // 2)
    per = 2 * heads // owners
    vmem, dma = pltpu.VMEM, pltpu.SemaphoreType.DMA
    attn, ga, up = pl.pallas_call(
        functools.partial(step_kernel, counts),
        out_shape=(
            vmem(output_cotangent.shape, BF16),
            vmem((rank, width), F32),
            vmem(query_up_map.shape, F32),
        ),
        in_specs=[hbm] * 9,
        out_specs=(vm,) * 3,
        scratch_shapes=[
            vmem(layer_input.shape, BF16),
            vmem((1, width), F32),
            vmem(codes.shape, jnp.int32),
            vmem(column_scale_quantized.shape, jnp.int32),
            vmem((1, block_second_scale.shape[0]), F32),
            vmem((rank, width), BF16),
            vmem(query_up_map.shape, BF16),
            vmem((1, rows), jnp.int32),
            vmem(output_cotangent.shape, BF16),
            vmem((24, blocks, 128), F32),
            vmem((8, blocks // 2, 128), F32),
            vmem((codes.shape[0] // 2, 1024), BF16),
            vmem((2, tokens, 1024), F32),
            vmem((8, 128, tokens), F32),
            vmem((tokens, width), BF16),
            vmem((HEAD_SIZE // 2, tokens), F32),
            vmem((HEAD_SIZE // 2, tokens), F32),
            vmem((2, 8, 16, tokens), F32),
            vmem((2, 8, 16, tokens), BF16),
            vmem((2, 8, 16, tokens), BF16),
            vmem((8, 16 * heads, tokens), F32),
            vmem((8, 16 * heads, tokens), BF16),
            vmem((8, 16 * heads, tokens), BF16),
            vmem((tokens, heads * 128), BF16),
            vmem((16, rows), BF16),
            vmem((chips, 16, tokens), BF16),
            vmem((chips, 2, tokens, 128), BF16),
            vmem((256, heads * tokens), BF16),
            vmem((128, heads * tokens), BF16),
            vmem((256 + 16, tokens), BF16),
            vmem((8 * heads, tokens), F32),
            vmem((heads, 256 + 16, tokens), F32),
            vmem((heads, 128 + 16, tokens), F32),
            vmem((heads, 128, tokens), BF16),
            vmem((heads, tokens, tokens), F32),
            vmem((heads, tokens, tokens), F32),
            vmem((heads, tokens, tokens), BF16),
            vmem((heads, tokens, tokens), BF16),
            vmem((tokens, heads * 128), BF16),
            vmem((rows, heads * 128), BF16),
            vmem((rank, tokens), F32),
            vmem((3, rank, tokens), F32),
            vmem((owners, per, rank, 128), BF16),
            vmem((chips, per, rank, 128), BF16),
            vmem((per, rank, 128), BF16),
            vmem((4 * owners, per, rank, 128), BF16),
            vmem((owners, per, 8, 128), F32),
            vmem((chips, per, 8, 128), F32),
            vmem((per, 8, 128), F32),
            vmem((2 * owners, per, 8, 128), F32),
            dma((10,)),
            dma((10,)),
            dma((10,)),
            dma((1,)),
            dma((2 * chips,)),
            dma((10,)),
        ],
        compiler_params=pltpu.CompilerParams(
            collective_id=0, has_side_effects=True, vmem_limit_bytes=56 * 1024 * 1024
        ),
        name="step",
    )(
        layer_input, gain[None, :], codes, column_scale_quantized, block_second_scale[None, :],
        query_down_map.T, query_up_map, token_document[None, :], output_cotangent,
    )
    attn, ga, up = pl.pallas_call(
        store_kernel,
        out_shape=tuple(jax.ShapeDtypeStruct(a.shape, a.dtype) for a in (attn, ga, up)),
        in_specs=[vm] * 3,
        out_specs=(hbm,) * 3,
        scratch_shapes=[dma((3,))],
        compiler_params=pltpu.CompilerParams(vmem_limit_bytes=4 * 1024 * 1024),
        name="store",
    )(attn, ga, up)
    return attn, ga.T, up


def solution(mesh):
    return jax.shard_map(
        functools.partial(on_device, (mesh.shape["ctx"], mesh.shape["fsdp"])),
        mesh=mesh,
        in_specs=(
            P("ctx", None),
            P(),
            P("fsdp", None),
            P("fsdp", None),
            P(),
            P(),
            P(None, "fsdp"),
            P("ctx"),
            P("ctx", "fsdp"),
        ),
        out_specs=(P("ctx", "fsdp"), P(), P(None, "fsdp")),
        check_vma=False,
    )
```

```python
import math
import functools

import jax
import jax.numpy as jnp
from jax import lax
from jax.experimental import pallas as pl
from jax.experimental.pallas import tpu as pltpu
from jax.sharding import PartitionSpec as P

HEAD_SIZE = 128
ADAPTER_SCALE = 2.0
ROPE_BASE = 500000.0
MESH = pl.DeviceIdType.MESH
F32 = jnp.float32
BF16 = jnp.bfloat16
I16 = jnp.int16

NF4_LEVELS = [
    -1.0,
    -0.6961928009986877,
    -0.5250730514526367,
    -0.39491748809814453,
    -0.28444138169288635,
    -0.18477343022823334,
    -0.09105003625154495,
    0.0,
    0.07958029955625534,
    0.16093020141124725,
    0.24611230194568634,
    0.33791524171829224,
    0.44070982933044434,
    0.5626170039176941,
    0.7229568362236023,
    1.0,
]


def take_lanes(values, index):
    return jnp.take_along_axis(values, index, axis=1, mode="promise_in_bounds")


GATHERED = (1, 3, 5, 7)
LANE_PICK = lax.GatherDimensionNumbers(
    offset_dims=(), collapsed_slice_dims=(1,), start_index_map=(1,),
    operand_batching_dims=(0,), start_indices_batching_dims=(0,),
)


def pick_lanes(values, index):
    return lax.gather(
        values, index[..., None], LANE_PICK, (1, 1),
        mode=lax.GatherScatterMode.PROMISE_IN_BOUNDS,
    )


def dot(a, b):
    return jnp.dot(a, b, preferred_element_type=F32)


def nt(a, b):
    return lax.dot_general(a, b, (((1,), (1,)), ((), ())), preferred_element_type=F32)


def tn(a, b):
    return lax.dot_general(a, b, (((0,), (0,)), ((), ())), preferred_element_type=F32)


def eye(size):
    row = lax.broadcasted_iota(jnp.int32, (size, size), 0)
    col = lax.broadcasted_iota(jnp.int32, (size, size), 1)
    return (row == col).astype(F32).astype(BF16)


def step_kernel(
    counts,
    x_hbm, gain_hbm, codes_hbm, cs_hbm, bss_hbm, qdown_hbm, qup_hbm, ids_hbm, do_hbm,
    out_ref, ga_out, up_out,
    x_ref, gain_ref, codes_ref, cs_ref, bss_ref, qdown_ref, qup_ref, ids_ref, do_ref, scl, vscl, weights, acc, acct, xn, cos_ref, sin_ref, own_kv, send_kv, recv_kv, own_q, send_q, recv_q,
    do_all, ids_own, ids_all, kv_all, queries, cotans, vk, row_max, out_acc, grad_acc, lin,
    score_buf, dots_buf, prob_buf, weight_buf, out_stage, out_in, mid_own, mid_in,
    ga_part, ga_in, ga_sum, ga_all, up_part, up_in, up_sum, up_all,
    load, pair_send, pair_recv, block_send, block_recv, sems,
):
    early = x_hbm.shape[0] // 2
    loads = [
        pltpu.make_async_copy(src, dst, load.at[number])
        for number, (src, dst) in enumerate(
            (
                (x_hbm.at[:early], x_ref.at[:early]), (gain_hbm, gain_ref), (ids_hbm, ids_ref),
                (do_hbm, do_ref),
                (bss_hbm, bss_ref), (cs_hbm, cs_ref), (codes_hbm, codes_ref),
                (qdown_hbm, qdown_ref), (qup_hbm, qup_ref), (x_hbm.at[early:], x_ref.at[early:]),
            )
        )
    ]
    for number in (0, 1, 9, 2, 3, 4, 5, 6, 7, 8):
        loads[number].start()
    ctx_count, fsdp_count = counts
    total = ctx_count * fsdp_count
    ctx, member = lax.axis_index("ctx"), lax.axis_index("fsdp")
    me = ctx * fsdp_count + member
    partner = 1 - member
    chip, core = ctx // 2, lax.rem(ctx, 2)
    outer, inner = chip // 2, lax.rem(chip, 2)
    sibling = ctx + 1 - 2 * core
    chips = ctx_count // 2
    rows, width = x_ref.shape
    tokens = 2 * rows
    depth = codes_ref.shape[0]
    half_depth = depth // 2
    blocks = cs_ref.shape[0]
    block_rows = depth // blocks
    half_blocks = blocks // 2

    barrier = pltpu.get_barrier_semaphore()

    low = chip < chips // 2

    def far_first(step, count):
        return jnp.where(low, count - 1 - step, step)

    def greet(step, carry):
        other = far_first(step, total)

        @pl.when(other != me)
        def _():
            pl.semaphore_signal(
                barrier, inc=1, device_id=(other // fsdp_count, lax.rem(other, fsdp_count)),
                device_id_type=MESH,
            )

        return carry

    lax.fori_loop(0, total, greet, 0)

    mine_at = pl.multiple_of(core * rows, rows)
    other_at = pl.multiple_of((1 - core) * rows, rows)
    loads[0].wait()
    loads[1].wait()
    for r in range(0, rows, 16):
        if r == early:
            loads[9].wait()
        wide = x_ref[r : r + 16, :].astype(F32)
        inverse = lax.rsqrt(jnp.mean(wide * wide, axis=-1, keepdims=True) + 1e-05)
        xn[pl.ds(pl.multiple_of(mine_at + r, 16), 16), :] = (
            wide * inverse * gain_ref[...]
        ).astype(BF16)
    loads[2].wait()
    ids_own[...] = jnp.broadcast_to(
        ids_ref[...].astype(F32), (16, rows)
    ).astype(BF16)
    half_columns = do_ref.shape[1] // 2
    mine_columns = pl.multiple_of(core * half_columns, 128)
    other_columns = pl.multiple_of((1 - core) * half_columns, 128)
    loads[3].wait()
    do_all[pl.ds(mine_at, rows), :] = do_ref[:, pl.ds(mine_columns, half_columns)]

    lane = lax.broadcasted_iota(jnp.int32, (blocks, 128), 1)
    loads[4].wait()
    loads[5].wait()
    all_blocks = bss_ref.shape[1]
    scale_row = lax.broadcasted_iota(jnp.int32, (blocks, all_blocks), 0) + member * blocks
    scale_lane = lax.broadcasted_iota(jnp.int32, (blocks, all_blocks), 1)
    second = jnp.sum(
        jnp.where(scale_row == scale_lane, bss_ref[...], 0.0), axis=1, keepdims=True
    )
    for tile in range(3):
        source = [
            (cs_ref[:, tile * 1024 + m * 128 : tile * 1024 + (m + 1) * 128].astype(F32) + 1.0)
            / 256.0
            * second
            for m in range(8)
        ]
        for n in range(8):
            index = 8 * (lane % 16) + n
            picked = take_lanes(source[0], index)
            for m in range(1, 8):
                picked = jnp.where(lane // 16 == m, take_lanes(source[m], index), picked)
            scl[tile * 8 + n] = picked

    pl.semaphore_wait(barrier, total - 1)

    def pair_copy(src, dst, number, device):
        copy = pltpu.make_async_remote_copy(
            src_ref=src, dst_ref=dst, send_sem=pair_send.at[number],
            recv_sem=pair_recv.at[number], device_id=device, device_id_type=MESH,
        )
        copy.start()
        return copy

    across = (sibling, member)
    beside = (ctx, partner)
    span = pl.ds(mine_at, rows)
    near = xn.at[span, pl.ds(pl.multiple_of(member * depth, 128), depth)]
    far = xn.at[span, pl.ds(pl.multiple_of(partner * depth, 128), depth)]
    copy_x = pair_copy(near, near, 0, across)
    copy_x_rest = pair_copy(far, far, 1, across)
    copy_do = pair_copy(
        do_ref.at[:, pl.ds(other_columns, half_columns)], do_all.at[span], 2, across
    )

    def send(src, dst, number, ctx_to, fsdp_to):
        pltpu.make_async_remote_copy(
            src_ref=src, dst_ref=dst, send_sem=sems.at[2 * number],
            recv_sem=sems.at[2 * number + 1], device_id=(ctx_to, fsdp_to),
            device_id_type=MESH,
        ).start()

    def hold(src, dst, number):
        pltpu.make_async_copy(src, dst, sems.at[2 * number + 1]).start()

    def await_all(buffer, number):
        pltpu.make_async_copy(buffer, buffer, sems.at[2 * number + 1]).wait()

    def tell_ids(step, carry):
        send(ids_own, ids_all.at[chip, :, span], 4, lax.rem(ctx + step, ctx_count), member)
        return carry

    lax.fori_loop(1, ctx_count, tell_ids, 0)

    pr = lax.broadcasted_iota(jnp.int32, (128, 128), 0)
    pd = lax.broadcasted_iota(jnp.int32, (128, 128), 1)
    perm = (pd == 8 * (pr % 16) + pr // 16).astype(F32).astype(BF16)
    eye_wide = eye(256)

    chunk = 512
    per_chunk = chunk // block_rows
    short_lane = lax.broadcasted_iota(jnp.int32, (block_rows, 128), 1)
    half_lane = lax.broadcasted_iota(jnp.int32, (half_blocks, 128), 1)
    long_lane = lax.broadcasted_iota(jnp.int32, (tokens, 128), 1)
    levels = [jnp.full((block_rows, 128), level, BF16) for level in NF4_LEVELS]
    table = jnp.zeros((block_rows, 128), F32)
    for code, level in enumerate(NF4_LEVELS):
        table = jnp.where(short_lane % 16 == code, F32(level), table)

    def phase(paired, tile, half, ready=None):
        if paired:
            shift = 16 + 96 * core

            def chosen(lanes):
                return lax.rem(lanes // 16, 2) == core

            def words_at(at):
                return jnp.where(
                    short_lane < 64,
                    codes_ref[pl.ds(at, block_rows), 128:256],
                    codes_ref[pl.ds(at, block_rows), 256:384],
                )
        else:
            shift = 64
            tile_at = pl.multiple_of(tile * 128, 128)

            def chosen(lanes):
                return lanes // 64 == half

            def words_at(at):
                return codes_ref[pl.ds(at, block_rows), pl.ds(tile_at, 128)]

        for n in range(8):
            if paired:
                scale = jnp.where(lane < 64, scl[8 + n], scl[16 + n])
            else:
                scale = scl[tile * 8 + n]
            vscl[n] = jnp.where(
                chosen(half_lane), scale[:half_blocks], pltpu.roll(scale[half_blocks:], shift, 1)
            )
        if ready is None:
            acc[...] = jnp.zeros_like(acc)
        first = chosen(short_lane)

        def step(k, carry):
            if ready is None:
                at = pl.multiple_of(member * depth + k * chunk, 128)
                lower = xn[:, pl.ds(at, chunk)]
                upper = xn[:, pl.ds(pl.multiple_of(at + half_depth, 128), chunk)]
            low_words, high_words, full_words = [], [], []
            for b in range(per_chunk):
                row = pl.multiple_of(k * chunk + b * block_rows, block_rows)
                words = jnp.where(
                    first,
                    words_at(row),
                    pltpu.roll(words_at(pl.multiple_of(row + half_depth, block_rows)), shift, 1),
                )
                full_words.append(words)
                low_words.append(words.astype(I16))
                high_words.append(jnp.right_shift(words, 16).astype(I16))
            for pair in range(4):
                planes = []
                for n in (2 * pair, 2 * pair + 1):
                    pieces = []
                    for b in range(per_chunk):
                        scale = vscl[n, pl.ds(k * per_chunk + b, 1), :]
                        if n % 8 in GATHERED:
                            code = jnp.bitwise_and(jnp.right_shift(full_words[b], 4 * n), 15)
                            pieces.append((pick_lanes(table, code) * scale).astype(BF16))
                            continue
                        words = low_words[b] if n < 4 else high_words[b]
                        values = levels
                        for bit in range(4):
                            place = 4 * (n % 4) + bit
                            mark = 1 << place if place < 15 else -(1 << 15)
                            mask = (words & jnp.int16(mark)) != 0
                            values = [
                                jnp.where(mask, values[v + 1], values[v])
                                for v in range(0, len(values), 2)
                            ]
                        pieces.append(values[0] * scale.astype(BF16))
                    planes.append(jnp.concatenate(pieces, axis=0))
                weight = jnp.concatenate(planes, axis=1)
                columns = slice(pair * 256, (pair + 1) * 256)
                if ready is None:
                    acc[0, :, columns] += dot(lower, weight)
                    acc[1, :, columns] += dot(upper, weight)
                else:
                    weights[pl.ds(pl.multiple_of(k * chunk, chunk), chunk), columns] = weight
            return carry

        lax.fori_loop(0, half_depth // chunk, step, 0)
        if ready is not None:
            ready()
            for side in range(2):
                at = pl.multiple_of(member * depth + side * half_depth, 128)
                for pair in range(4):
                    columns = slice(pair * 256, (pair + 1) * 256)
                    acc[side, :, columns] = dot(xn[:, pl.ds(at, half_depth)], weights[:, columns])
        keep = chosen(long_lane)
        for n in range(8):
            columns = slice(n * 128, (n + 1) * 128)
            acct[n] = jnp.where(keep, acc[0, :, columns], acc[1, :, columns]).T

    loads[6].wait()

    def kv_field(group, part):
        at = pl.multiple_of(64 * group, 64) + 32 * part
        return acct[:, pl.ds(pl.multiple_of(at, 32), 16), :] + acct[
            :, pl.ds(pl.multiple_of(at + 16, 16), 16), :
        ]

    phase(True, 0, 0, copy_x.wait)
    copy_kv = [None, None]
    for part in (1, 0):
        send_kv[part] = kv_field(partner, part).astype(BF16)
        copy_kv[part] = pair_copy(send_kv.at[part], recv_kv.at[part], 3 + 6 * part, beside)
    for part in range(2):
        own_kv[part] = kv_field(member, part)

    place = 3 * partner + core
    phase(False, place // 2, lax.rem(place, 2))
    send_q[...] = (acct[:, :64, :] + acct[:, 64:, :]).astype(BF16)
    copy_q = pair_copy(send_q, recv_q, 4, beside)

    at = lax.broadcasted_iota(jnp.int32, (64, tokens), 0)
    feature = (8 * (at % 8) + at // 8).astype(F32)
    position = (lax.broadcasted_iota(jnp.int32, (64, tokens), 1) + chip * tokens).astype(F32)
    angle = position * jnp.exp(feature * (-2.0 * math.log(ROPE_BASE) / HEAD_SIZE))
    cos_ref[...] = jnp.cos(angle)
    sin_ref[...] = jnp.sin(angle)

    loads[7].wait()
    loads[8].wait()
    copy_x_rest.wait()
    lr_t = nt(qdown_ref[...], xn[...]).astype(BF16)
    copy_do.wait()
    hold(ids_own, ids_all.at[chip, :, span], 4)
    await_all(ids_all, 4)
    my_ids = ids_all[chip]
    heads = own_q.shape[1] // 16
    local = pl.multiple_of(core * heads * 128, 128)
    marks = lax.broadcasted_iota(jnp.int32, (128, tokens), 0).astype(F32)
    tags = (marks == jnp.broadcast_to(my_ids[:1].astype(F32), (128, tokens))).astype(F32)
    tags = tags.astype(BF16)
    for head in range(heads):
        columns = slice(head * tokens, (head + 1) * tokens)
        queries[128:, columns] = tags
        cotans[:, columns] = nt(perm, do_all[:, head * 128 : (head + 1) * 128]).astype(BF16)

    cosine = cos_ref[...].reshape(8, 8, tokens)
    sine = sin_ref[...].reshape(8, 8, tokens)

    def rotate(field):
        a, b = field[:, :8, :], field[:, 8:, :]
        return jnp.concatenate([a * cosine - b * sine, b * cosine + a * sine], axis=1)

    has_next = outer + 1 < chips // 2

    def send_block(block, part, to_chip):
        half = kv_all.at[block, part]
        pltpu.make_async_remote_copy(
            src_ref=half, dst_ref=half,
            send_sem=block_send.at[0], recv_sem=block_recv.at[2 * block + part],
            device_id=(2 * to_chip + core, member), device_id_type=MESH,
        ).start()

    def await_block(block, part):
        half = kv_all.at[block, part]
        pltpu.make_async_copy(half, half, block_recv.at[2 * block + part]).wait()

    def relay(ahead, parts=(0, 1)):
        block = 2 * (outer - 1 - ahead) + inner
        for part in parts:
            await_block(block, part)

            @pl.when(has_next)
            def _():
                send_block(block, part, chip + 2)

            send_block(block, part, 2 * outer + 1 - inner)

    eye_half = eye(128)
    for part in (1, 0):
        copy_kv[part].wait()
        field = own_kv[part] + recv_kv[part].astype(F32)
        if part == 0:
            field = rotate(field)
        field = field.reshape(128, tokens).astype(BF16)
        kv_all[chip, 1 - part] = tn(field, eye_half).astype(BF16)

        @pl.when(has_next)
        def _():
            send_block(chip, 1 - part, chip + 2)

        @pl.when(inner == 0)
        def _():
            send_block(chip, 1 - part, chip + 1)

    @pl.when(outer > 0)
    def _():
        relay(0)

    place = 3 * member + core
    phase(False, place // 2, lax.rem(place, 2))
    own_q[...] = acct[:, :64, :] + acct[:, 64:, :]

    @pl.when(outer > 1)
    def _():
        relay(1, (0,))

    copy_q.wait()
    for head in range(heads):
        columns = slice(head * tokens, (head + 1) * tokens)
        up_cols = qup_ref[:, pl.ds(pl.multiple_of(local + head * 128, 128), 128)]
        adapter = dot(nt(perm, up_cols).astype(BF16), lr_t).reshape(8, 16, tokens)
        query = own_q[:, 16 * head : 16 * head + 16, :]
        query = query + recv_q[:, 16 * head : 16 * head + 16, :].astype(F32)
        query = query + ADAPTER_SCALE * adapter
        queries[:128, columns] = rotate(query).reshape(128, tokens).astype(BF16)

    @pl.when(outer > 1)
    def _():
        relay(1, (1,))

    soft_scale = 1.0 / math.sqrt(HEAD_SIZE)
    log_scale = soft_scale / math.log(2.0)
    tag_row = lax.broadcasted_iota(jnp.int32, (16, tokens), 0).astype(F32)
    spread_row = lax.broadcasted_iota(jnp.int32, (16, 128), 0)
    spread_lane = lax.broadcasted_iota(jnp.int32, (16, 128), 1)
    spread_tags = (spread_row == spread_lane).astype(F32).astype(BF16)
    vk[256:, :] = jnp.ones((16, tokens), BF16)

    def attend(block, diagonal):
        both = jnp.concatenate([kv_all[block, 0], kv_all[block, 1]], axis=1)
        block_ids = ids_all[block].astype(F32)
        barred = jnp.where(block_ids == tag_row, 0.0, -1e30).astype(BF16)
        barred = tn(barred, spread_tags).astype(BF16)
        lhs = jnp.concatenate([both[:, 128:], barred], axis=1)
        vk[:256, :] = nt(eye_wide, both).astype(BF16)
        tops, decays = [], []
        for head in range(heads):
            columns = slice(head * tokens, (head + 1) * tokens)
            scores = dot(lhs, queries[:, columns]) * log_scale
            if diagonal:
                ki = lax.broadcasted_iota(jnp.int32, (tokens, tokens), 0)
                qi = lax.broadcasted_iota(jnp.int32, (tokens, tokens), 1)
                scores = jnp.where(ki <= qi, scores, -1e30)
            score_buf[head] = scores
            tops.append(jnp.max(scores, axis=0, keepdims=True))
            dots_buf[head] = dot(both[:, :128], cotans[:, columns])
        for head in range(heads):
            row = slice(8 * head, 8 * head + 1)
            top = tops[head]
            if not diagonal:
                before = row_max[row, :]
                top = jnp.maximum(top, before)
                decays.append(jnp.exp2(before - top))
            row_max[row, :] = top
            expo = jnp.exp2(score_buf[head] - top)
            prob_buf[head] = expo.astype(BF16)
            weight_buf[head] = (expo * dots_buf[head]).astype(BF16)
        for head in range(heads):
            new_out = dot(vk[...], prob_buf[head])
            new_grad = dot(vk[128:, :], weight_buf[head])
            if diagonal:
                out_acc[head] = new_out
                grad_acc[head] = new_grad
            else:
                decay = decays[head]
                out_acc[head] = decay * out_acc[head] + new_out
                grad_acc[head] = decay * grad_acc[head] + new_grad

    attend(chip, True)

    def visit(step, carry):
        place = step - inner
        odd = lax.rem(place + 2, 2) == 1
        ahead = step // 2 + 1

        @pl.when((lax.rem(step, 2) == 0) & (ahead > 1) & (ahead < outer))
        def _():
            relay(ahead)

        crossed = 2 * (outer - 1 - (place - 1) // 2) + 1 - inner
        crossed = jnp.where(place < 0, chip - 1, crossed)
        column = 2 * (outer - 1 - place // 2) + inner
        block = jnp.where(odd, crossed, column)

        @pl.when(odd)
        def _():
            await_block(block, 0)
            await_block(block, 1)

        attend(block, False)
        return carry

    lax.fori_loop(0, chip, visit, 0)

    middle = jnp.zeros((16, tokens), F32)
    for head in range(heads):
        inverse = 1.0 / out_acc[head, 256:257, :]
        mean_dot = grad_acc[head, 128:129, :] * inverse
        grad = grad_acc[head, :128, :] - mean_dot * out_acc[head, 128:256, :]
        grad = (soft_scale * inverse * grad).reshape(8, 16, tokens)
        a, b = grad[:, :8, :], grad[:, 8:, :]
        turned = jnp.concatenate([a * cosine + b * sine, b * cosine - a * sine], axis=1)
        lin_t = turned.reshape(128, tokens).astype(BF16)
        lin[head] = lin_t
        up_cols = qup_ref[:, pl.ds(pl.multiple_of(local + head * 128, 128), 128)]
        middle = middle + dot(nt(up_cols, perm).astype(BF16), lin_t)
    mid_own[...] = middle
    quarter = 2 * core + member
    mid_copies = [
        pair_copy(mid_own, mid_in.at[number], 6 + number, device)
        for number, device in enumerate(((ctx, partner), (sibling, partner), (sibling, member)))
    ]

    owners, per = up_part.shape[:2]
    stride = chips // 2 // owners
    first_owner = chips // 4
    turn = chip - first_owner
    mine = turn // stride
    owner = (turn >= 0) & (turn < owners * stride) & (lax.rem(turn + chips, stride) == 0)
    up_slot = core * owners + mine
    ga_slot = quarter * owners + mine
    back = 16 * (pd % 8) + pd // 8
    for head in range(heads):
        up = take_lanes(ADAPTER_SCALE * nt(lr_t, lin[head]), back[:16])
        for part in range(2):
            piece = 2 * head + part
            up_part[piece // per, piece % per] = up[8 * part : 8 * part + 8]

    def scatter(part, into, number):
        def one(step, carry):
            j = far_first(step, owners)
            to = first_owner + j * stride

            @pl.when(to != chip)
            def _():
                send(part.at[j], into.at[chip], number, 2 * to + core, member)

            return carry

        lax.fori_loop(0, owners, one, 0)

        @pl.when(owner)
        def _():
            hold(part.at[mine], into.at[chip], number)

    scatter(up_part, up_in, 0)

    for head in range(heads):
        inverse = 1.0 / out_acc[head, 256:257, :]
        out = (out_acc[head, :128, :] * inverse).astype(BF16)
        out_stage[:, head * 128 : (head + 1) * 128] = tn(out, perm).astype(BF16)

    for copy in mid_copies:
        copy.wait()
    middle = mid_own[...] + mid_in[0] + mid_in[1] + mid_in[2]
    middle = (ADAPTER_SCALE * middle).astype(BF16)
    share = owners * per * 128
    ga = dot(middle, xn[:, pl.ds(pl.multiple_of(quarter * share, 128), share)])
    for j in range(owners * per):
        ga_part[j // per, j % per] = ga[:, j * 128 : (j + 1) * 128].astype(BF16)
    scatter(ga_part, ga_in, 1)

    copy_out = pair_copy(out_stage.at[pl.ds(other_at, rows)], out_in, 5, across)
    out_ref[:, pl.ds(mine_columns, half_columns)] = out_stage[pl.ds(mine_at, rows), :]

    @pl.when(owner)
    def _():
        await_all(up_in, 0)
        up_sum[...] = jnp.sum(up_in[...], axis=0)

        def spread_up(step, carry):
            to = far_first(step, ctx_count)

            @pl.when(to != ctx)
            def _():
                send(up_sum, up_all.at[up_slot], 2, to, member)

            return carry

        lax.fori_loop(0, ctx_count, spread_up, 0)
        hold(up_sum, up_all.at[up_slot], 2)

        await_all(ga_in, 1)
        ga_sum[...] = jnp.sum(ga_in[...].astype(F32), axis=0).astype(BF16)

        def spread_ga(step, carry):
            place = far_first(step, total)
            to, to_fsdp = place // fsdp_count, lax.rem(place, fsdp_count)

            @pl.when(place != me)
            def _():
                send(ga_sum, ga_all.at[ga_slot], 3, to, to_fsdp)

            return carry

        lax.fori_loop(0, total, spread_ga, 0)
        hold(ga_sum, ga_all.at[ga_slot], 3)

    copy_out.wait()
    out_ref[:, pl.ds(other_columns, half_columns)] = out_in[...]

    await_all(up_all, 2)
    for j in range(2 * owners * per):
        row, col = 8 * (j % 2), 128 * (j // 2)
        up_out[row : row + 8, col : col + 128] = up_all[j // per, j % per]
    await_all(ga_all, 3)
    for j in range(4 * owners * per):
        ga_out[:, j * 128 : (j + 1) * 128] = ga_all[j // per, j % per].astype(F32)

    def drain(buffer, semaphore, sent):
        def one(step, carry):
            pltpu.make_async_copy(buffer, buffer, semaphore).wait()
            return carry

        lax.fori_loop(0, sent, one, 0)

    onward = has_next.astype(jnp.int32)
    passed = 2 * (onward + 1 - inner + outer * (onward + 1))
    drain(kv_all.at[chip, 0], block_send.at[0], passed)
    scattered = owners - owner.astype(jnp.int32)
    drain(up_part.at[0], sems.at[0], scattered)
    drain(ga_part.at[0], sems.at[2], scattered)
    drain(up_sum, sems.at[4], jnp.where(owner, ctx_count - 1, 0))
    drain(ga_sum, sems.at[6], jnp.where(owner, total - 1, 0))
    drain(ids_own, sems.at[8], ctx_count - 1)


def store_kernel(attn_ref, ga_ref, up_ref, attn_out, ga_out, up_out, sems):
    copies = [
        pltpu.make_async_copy(src, dst, sems.at[number])
        for number, (src, dst) in enumerate(
            ((attn_ref, attn_out), (ga_ref, ga_out), (up_ref, up_out))
        )
    ]
    for copy in copies:
        copy.start()
    for copy in copies:
        copy.wait()


def on_device(
    counts, layer_input, gain, codes, column_scale_quantized, block_second_scale,
    query_down_map, query_up_map, token_document, output_cotangent,
):
    ctx_count, fsdp_count = counts
    total = ctx_count * fsdp_count
    chips = ctx_count // 2
    rows, width = layer_input.shape
    tokens = 2 * rows
    vm = pl.BlockSpec(memory_space=pltpu.VMEM)
    hbm = pl.BlockSpec(memory_space=pltpu.HBM)
    blocks = column_scale_quantized.shape[0]
    rank, local_columns = query_up_map.shape
    heads = local_columns // HEAD_SIZE // 2
    owners = math.gcd(2 * heads, chips // 2)
    per = 2 * heads // owners
    vmem, dma = pltpu.VMEM, pltpu.SemaphoreType.DMA
    attn, ga, up = pl.pallas_call(
        functools.partial(step_kernel, counts),
        out_shape=(
            vmem(output_cotangent.shape, BF16),
            vmem((rank, width), F32),
            vmem(query_up_map.shape, F32),
        ),
        in_specs=[hbm] * 9,
        out_specs=(vm,) * 3,
        scratch_shapes=[
            vmem(layer_input.shape, BF16),
            vmem((1, width), F32),
            vmem(codes.shape, jnp.int32),
            vmem(column_scale_quantized.shape, jnp.int32),
            vmem((1, block_second_scale.shape[0]), F32),
            vmem((rank, width), BF16),
            vmem(query_up_map.shape, BF16),
            vmem((1, rows), jnp.int32),
            vmem(output_cotangent.shape, BF16),
            vmem((24, blocks, 128), F32),
            vmem((8, blocks // 2, 128), F32),
            vmem((codes.shape[0] // 2, 1024), BF16),
            vmem((2, tokens, 1024), F32),
            vmem((8, 128, tokens), F32),
            vmem((tokens, width), BF16),
            vmem((HEAD_SIZE // 2, tokens), F32),
            vmem((HEAD_SIZE // 2, tokens), F32),
            vmem((2, 8, 16, tokens), F32),
            vmem((2, 8, 16, tokens), BF16),
            vmem((2, 8, 16, tokens), BF16),
            vmem((8, 16 * heads, tokens), F32),
            vmem((8, 16 * heads, tokens), BF16),
            vmem((8, 16 * heads, tokens), BF16),
            vmem((tokens, heads * 128), BF16),
            vmem((16, rows), BF16),
            vmem((chips, 16, tokens), BF16),
            vmem((chips, 2, tokens, 128), BF16),
            vmem((256, heads * tokens), BF16),
            vmem((128, heads * tokens), BF16),
            vmem((256 + 16, tokens), BF16),
            vmem((8 * heads, tokens), F32),
            vmem((heads, 256 + 16, tokens), F32),
            vmem((heads, 128 + 16, tokens), F32),
            vmem((heads, 128, tokens), BF16),
            vmem((heads, tokens, tokens), F32),
            vmem((heads, tokens, tokens), F32),
            vmem((heads, tokens, tokens), BF16),
            vmem((heads, tokens, tokens), BF16),
            vmem((tokens, heads * 128), BF16),
            vmem((rows, heads * 128), BF16),
            vmem((rank, tokens), F32),
            vmem((3, rank, tokens), F32),
            vmem((owners, per, rank, 128), BF16),
            vmem((chips, per, rank, 128), BF16),
            vmem((per, rank, 128), BF16),
            vmem((4 * owners, per, rank, 128), BF16),
            vmem((owners, per, 8, 128), F32),
            vmem((chips, per, 8, 128), F32),
            vmem((per, 8, 128), F32),
            vmem((2 * owners, per, 8, 128), F32),
            dma((10,)),
            dma((10,)),
            dma((10,)),
            dma((1,)),
            dma((2 * chips,)),
            dma((10,)),
        ],
        compiler_params=pltpu.CompilerParams(
            collective_id=0, has_side_effects=True, vmem_limit_bytes=56 * 1024 * 1024
        ),
        name="step",
    )(
        layer_input, gain[None, :], codes, column_scale_quantized, block_second_scale[None, :],
        query_down_map.T, query_up_map, token_document[None, :], output_cotangent,
    )
    attn, ga, up = pl.pallas_call(
        store_kernel,
        out_shape=tuple(jax.ShapeDtypeStruct(a.shape, a.dtype) for a in (attn, ga, up)),
        in_specs=[vm] * 3,
        out_specs=(hbm,) * 3,
        scratch_shapes=[dma((3,))],
        compiler_params=pltpu.CompilerParams(vmem_limit_bytes=4 * 1024 * 1024),
        name="store",
    )(attn, ga, up)
    return attn, ga.T, up


def solution(mesh):
    return jax.shard_map(
        functools.partial(on_device, (mesh.shape["ctx"], mesh.shape["fsdp"])),
        mesh=mesh,
        in_specs=(
            P("ctx", None),
            P(),
            P("fsdp", None),
            P("fsdp", None),
            P(),
            P(),
            P(None, "fsdp"),
            P("ctx"),
            P("ctx", "fsdp"),
        ),
        out_specs=(P("ctx", "fsdp"), P(), P(None, "fsdp")),
        check_vma=False,
    )
```
